256 devices in a mesh: row: 8 (over y, core), col: 32 (over z, x).
Axes of the slice: x: 4, y: 4, z: 8, core: 2. Of those that a mesh axis runs over, the one named last changes fastest.
Arguments:
- factor: float32 [6, 2048, 6, 2048], P(None, 'row', None, 'col'), may hold values from -0.0625 to 0.0625
- diag_inv: float32 [6, 2048, 2048], P(None, None, 'row'), may hold values from -2 to 2, as said below
- structure: int32 [6, 6, 16], P(None, None, 'row'), may hold values 0 or 1
- parent: int32 [6], replicated, may hold values from 1 to 6, as said below
- post: float32 [6, 2048, 64], P(None, 'row', 'col'), may hold values from -6 to 6
Outputs:
- mean_x: float32 [6, 2048, 64], P(None, 'row', 'col')
- variance: float32 [6, 2048], P(None, 'row')
The draws below stay inside these ranges and needn't reach their ends.
Inputs may be any that keep to these rules, and one draw needn't show every extreme that they name: parent[s] > s for s < 5, and parent[5] = 6; every supernode has at most 2 ancestors, and some supernode has exactly that many. The diagonal of each diag_inv[s] lies in 0.5 to 2.
All inputs are finite; a program needn't handle non-finite values. No bound on the sum of `structure` on one device may be relied on, other than what follows from the above.
Results may differ from the reference program's by a relative error of at most 0.00014.
Values sent between devices are 32-bit elements; how exact they have to be, the bound alone decides.
A program may use at most 128 MiB of HBM per device.

```python
import math
import jax
import jax.numpy as jnp
from jax import lax

W = 2048
NSUP = 6
LEVELS = 3
RB = 128
NRHS = 64
NBLK = 16


def draw_diag_inv(key, part):
    key_lower = jax.random.fold_in(key, 11)
    key_diagonal = jax.random.fold_in(key, 12)
    lower_part = jax.random.truncated_normal(key_lower, -4.0, 4.0, (NSUP, W, W), jnp.float32) * (0.5 / math.sqrt(W))
    diagonal = jnp.exp(jax.random.uniform(key_diagonal, (NSUP, W), jnp.float32, math.log(0.5), math.log(2.0)))
    identity = jnp.eye(W, dtype=jnp.float32)
    return lower_part * (1.0 - identity) + diagonal[:, :, None] * identity


def draw_parent(key, part):
    slot_ids = jnp.arange(NSUP + 1, dtype=jnp.int32)
    parent = jnp.full((NSUP,), NSUP, jnp.int32)
    depths = jnp.zeros((NSUP + 1,), jnp.int32)
    for member in range(NSUP - 2, -1, -1):
        if member >= NSUP - LEVELS:
            chosen = jnp.int32(member + 1)
        else:
            eligible = ((slot_ids > member) & (slot_ids < NSUP) & (depths <= LEVELS - 2)).astype(jnp.int32)
            eligible_count = jnp.sum(eligible)
            drawn_slot = jax.random.randint(jax.random.fold_in(key, member), (), 0, eligible_count)
            running = jnp.cumsum(eligible)
            chosen = jnp.argmax((running == drawn_slot + 1) & (eligible == 1)).astype(jnp.int32)
        parent = parent.at[member].set(chosen)
        depths = depths.at[member].set(depths[chosen] + 1)
    return parent


def plant(array, stream_key, low, high):
    spot = [jax.random.randint(jax.random.fold_in(stream_key, axis), (), 0, length) for axis, length in enumerate(array.shape)]
    widest = array.shape.index(max(array.shape))
    neighbour = spot[:widest] + [(spot[widest] + 1) % array.shape[widest]] + spot[widest + 1:]
    return array.at[tuple(spot)].set(low).at[tuple(neighbour)].set(high)


def steps_of(stream_key, dims, shards, smallest, high):
    gain, own = 1.0, jax.random.fold_in(stream_key, 6)
    for position, shards_of in shards:
        draws = jnp.exp(jax.random.uniform(jax.random.fold_in(own, position), (shards_of,), jnp.float32, smallest / len(shards), high / len(shards)))
        gain = gain * jnp.repeat(draws, dims[position] // shards_of).reshape([-1 if axis == position else 1 for axis in range(len(dims))])
    return gain


def gaussian(rng, extent, spread, bound, shards=(), held_as=jnp.bfloat16):
    result = spread * jax.random.normal(rng, extent, jnp.float32)
    if shards:
        result = result * steps_of(rng, extent, shards, -0.22, 0.18)
    return jnp.clip(result, -bound, bound).astype(held_as)


def setup_inputs(seed: int = 0) -> dict:
    key_of = jax.random.split(jax.random.key(seed), 6)
    return {
        "factor": gaussian(key_of[0], (NSUP, W, NSUP, W), (4 * W) ** -0.5, 0.0625, ((1, 8), (3, 32)), jnp.float32),
        "diag_inv": draw_diag_inv(jax.random.fold_in(key_of[5], 71), 0),
        "structure": plant((jax.random.randint(key_of[2], (NSUP, NSUP, NBLK), 0, 4) < 3).astype(jnp.int32), jax.random.fold_in(key_of[2], 1), 0, 1),
        "parent": draw_parent(jax.random.fold_in(key_of[5], 71), 0),
        "post": gaussian(key_of[4], (NSUP, W, NRHS), 1.0, 6.0, ((1, 8), (2, 32)), jnp.float32),
    }


def ancestor_table(parent, super_count):
    extended = jnp.concatenate([parent, jnp.full((1,), super_count, jnp.int32)])
    slot_ids = jnp.arange(super_count + 1, dtype=jnp.int32)
    targets = jnp.arange(super_count, dtype=jnp.int32)
    current = parent
    table = jnp.zeros((super_count, super_count), jnp.float32)
    for hop_index in range(super_count - 1):
        table = table + (current[:, None] == targets[None, :]).astype(jnp.float32)
        onehot = (current[:, None] == slot_ids[None, :]).astype(jnp.int32)
        current = jnp.sum(onehot * extended[None, :], axis=1).astype(jnp.int32)
    return table


def reference(factor, diag_inv, structure, parent, post):
    ancestry = ancestor_table(parent, NSUP)
    row_mask = jnp.repeat(structure.astype(jnp.float32), RB, axis=2) * ancestry[:, :, None]
    lower_inv = jnp.tril(diag_inv)
    order_total = NSUP * W
    solved = [None] * NSUP
    for current_sup in range(NSUP - 1, -1, -1):
        unit_rows = jnp.eye(W, order_total, k=current_sup * W, dtype=jnp.float32)
        right = jnp.concatenate([post[current_sup], unit_rows], axis=1)
        for later in range(current_sup + 1, NSUP):
            block = factor[later, :, current_sup, :] * row_mask[current_sup, later][:, None]
            right = right - jnp.dot(block.T, solved[later], precision=lax.Precision.HIGHEST, preferred_element_type=jnp.float32)
        solved[current_sup] = jnp.dot(lower_inv[current_sup].T, right, precision=lax.Precision.HIGHEST, preferred_element_type=jnp.float32)
    solution = jnp.stack(solved)
    mean_x = solution[:, :, :NRHS]
    unit_part = solution[:, :, NRHS:]
    variance = jnp.sum(unit_part * unit_part, axis=2)
    return mean_x, variance
```

```python
import functools

import jax
import jax.numpy as jnp
from jax import lax
from jax.experimental import pallas as pl
from jax.experimental.pallas import tpu as pltpu
from jax.sharding import Mesh
from jax.sharding import PartitionSpec as P

NS = 6
MESH = pl.DeviceIdType.MESH
F32 = jnp.float32
BF16 = jnp.bfloat16
GROUPS = (
    ((4, 0), (3, 0)),
    ((2, 0), (1, 0)),
    ((2, 1), (3, 1)),
    ((0, 1), (1, 1)),
    ((0, 0), None),
)
PLACE = {4: (0, 0), 2: (0, 1), 0: (0, 2), 3: (1, 0), 1: (1, 1), 5: (1, 2)}
NT = (((1,), (1,)), ((), ()))
NN = (((1,), (0,)), ((), ()))


def halves(value):
    high = value.astype(BF16)
    return high, (value - high.astype(F32)).astype(BF16)


def mm(left, right, dims=NN):
    return lax.dot_general(left, right, dims, preferred_element_type=F32)


def ancestor_of(parent, sup, second):
    first = parent[sup]
    if not second:
        return first
    return jnp.where(first < NS, parent[jnp.minimum(first, NS - 1)], NS)


def slot_of(step, side):
    if side == 0:
        sup = jnp.where(step == 0, 4, jnp.where(step <= 2, 2, 0))
    else:
        sup = jnp.where((step == 0) | (step == 2), 3, 1)
    return sup, (step == 2) | (step == 3)


def slot_target(parent, step, side):
    sup, second = slot_of(step, side)
    first = parent[sup]
    above = jnp.where(first < NS, parent[jnp.minimum(first, NS - 1)], NS)
    return sup, jnp.where(second, above, first)


def local_kernel(parent, marks, d_lo, d_hi, b_lo, b_hi, part, blocks):
    step = pl.program_id(0)
    row_at = lax.axis_index("y") * 2 + lax.axis_index("core")
    lane = lax.broadcasted_iota(jnp.int32, (64, 256), 1)
    nothing = jnp.zeros((64, 256), BF16)
    weights = []
    for side, b_ref in ((0, b_lo), (1, b_hi)):
        sup, target = slot_target(parent, step, side)
        valid = target < NS
        if side == 1:
            valid = valid & (step < 4)
        kept = jnp.minimum(target, NS - 1)
        first = jnp.where(valid, marks[sup, 0, kept], 0).astype(F32)
        second = jnp.where(valid, marks[sup, 1, kept], 0).astype(F32)
        block = b_ref[0, 0] * jnp.where(lane < 128, first, second)
        blocks[0, side] = block
        high, low = halves(block)
        if side == 0:
            weights.append(jnp.concatenate([high, nothing, low, nothing], axis=0))
            weights.append(jnp.concatenate([high, nothing, nothing, nothing], axis=0))
        else:
            weights.append(jnp.concatenate([nothing, high, nothing, low], axis=0))
            weights.append(jnp.concatenate([nothing, high, nothing, nothing], axis=0))
    row_of = lax.broadcasted_iota(jnp.int32, (256, 256), 0)
    col_of = lax.broadcasted_iota(jnp.int32, (256, 256), 1) + row_at * 256
    for piece in range(8):
        rows = pl.ds(piece * 256, 256)
        keep = row_of + piece * 256 >= col_of
        lo_high, lo_low = halves(jnp.where(keep, d_lo[0, rows, :], 0.0))
        hi_high, hi_low = halves(jnp.where(keep, d_hi[0, rows, :], 0.0))
        total = mm(lo_high, weights[0], NT) + mm(lo_low, weights[1], NT)
        total = total + mm(hi_high, weights[2], NT) + mm(hi_low, weights[3], NT)
        part[piece // 2, piece % 2, 0] = total[:, :128] + total[:, 128:]


def local_products(parent, marks, diag_inv, blocks):
    def d_map(side):
        def at(step, parent, marks):
            _, target = slot_target(parent, step, side)
            return jnp.minimum(target, NS - 1), 0, 0

        return at

    def b_map(side):
        def at(step, parent, marks):
            sup, target = slot_target(parent, step, side)
            return jnp.minimum(target, NS - 1), sup, 0, 0

        return at

    return pl.pallas_call(
        local_kernel,
        out_shape=(
            jax.ShapeDtypeStruct((4, 2, 5, 256, 128), F32),
            jax.ShapeDtypeStruct((5, 2, 64, 256), F32),
        ),
        grid_spec=pltpu.PrefetchScalarGridSpec(
            num_scalar_prefetch=2,
            grid=(5,),
            in_specs=[
                pl.BlockSpec((1, 2048, 256), d_map(0)),
                pl.BlockSpec((1, 2048, 256), d_map(1)),
                pl.BlockSpec((1, 1, 64, 256), b_map(0)),
                pl.BlockSpec((1, 1, 64, 256), b_map(1)),
            ],
            out_specs=[
                pl.BlockSpec((4, 2, 1, 256, 128), lambda step, parent, marks: (0, 0, step, 0, 0)),
                pl.BlockSpec((1, 2, 64, 256), lambda step, parent, marks: (step, 0, 0, 0)),
            ],
        ),
        compiler_params=pltpu.CompilerParams(vmem_limit_bytes=60_000_000),
        cost_estimate=pl.CostEstimate(flops=4_000_000_000, bytes_accessed=30_000_000, transcendentals=0),
    )(parent, marks, diag_inv, diag_inv, blocks, blocks)


class Sems:
    def __init__(self, ref):
        self.ref, self.used = ref, 0

    def take(self):
        self.used += 1
        return self.ref.at[self.used - 1]


def sweep_kernel(
    parent, part, blocks, diag_inv, post, mean_out, var_out,
    part1, part2, core1, core2, first1, first2, second1, second2, home1, home2, all1, all2,
    spread, d_raw, d_high, d_low, post_all, post_high, post_low, l_high, l_low, x_high, x_low,
    solved, block_buf, sums, sums_x, sums_z, own_var, sends, recvs, locals_,
):
    y, k = lax.axis_index("y"), lax.axis_index("core")
    z, x = lax.axis_index("z"), lax.axis_index("x")
    r, c = y * 2 + k, z * 4 + x
    up, down, over = (y + 1) % 4, (y + 3) % 4, (y + 2) % 4
    send_sems, recv_sems = Sems(sends), Sems(recvs)
    pending = []

    def copy_to(src, dst, device):
        copy = pltpu.make_async_remote_copy(
            src_ref=src, dst_ref=dst, send_sem=send_sems.take(), recv_sem=recv_sems.take(),
            device_id=device, device_id_type=MESH,
        )
        copy.start()
        pending.append(copy)
        return copy

    def drain():
        while pending:
            pending.pop().wait_send()

    load1 = pltpu.make_async_copy(part.at[:, :, pl.ds(0, 2)], part1, locals_.at[0])
    load1.start()
    d_loads = []
    for order, sup in enumerate((4, 3, 2, 1, 0, 5)):
        load = pltpu.make_async_copy(diag_inv.at[sup], d_raw.at[sup], locals_.at[1 + order])
        load.start()
        d_loads.append((sup, load))
    load2 = pltpu.make_async_copy(part.at[:, :, pl.ds(2, 3)], part2, locals_.at[7])
    load2.start()
    load_b = pltpu.make_async_copy(blocks, block_buf, locals_.at[8])
    load_b.start()

    barrier = pltpu.get_barrier_semaphore()

    def greet(step, carry):
        there = (c + step) % 32
        pl.semaphore_signal(barrier, inc=1, device_id=(y, k, there // 4, there % 4), device_id_type=MESH)
        return carry

    lax.fori_loop(1, 32, greet, 0)
    for device in ((up, k, z, x), (down, k, z, x), (y, 1 - k, z, x)):
        pl.semaphore_signal(barrier, inc=1, device_id=device, device_id_type=MESH)
    pl.semaphore_wait(barrier, 34)

    def to_columns(source, target):
        send_sem, recv_sem = send_sems.take(), recv_sems.take()

        def one(step, carry):
            there = (c + step) % 32
            pltpu.make_async_remote_copy(
                src_ref=source(there), dst_ref=target(c), send_sem=send_sem, recv_sem=recv_sem,
                device_id=(y, k, there // 4, there % 4), device_id_type=MESH,
            ).start()
            return carry

        lax.fori_loop(1, 32, one, 0)
        return send_sem, recv_sem

    def bulk(sources, target, sems):
        return pltpu.make_async_remote_copy(
            src_ref=sources, dst_ref=target, send_sem=sems[0], recv_sem=sems[1],
            device_id=(y, k, z, (x + 1) % 4), device_id_type=MESH,
        )

    def reduce_rows(group_count, mine, core, first, second, home):
        swap = copy_to(mine.at[:, 1 - k], core, (y, 1 - k, z, x))
        yield
        swap.wait_recv()
        core[over] += mine[over, k]
        one_up = copy_to(core.at[over, :, pl.ds(0, 128)], first.at[0], (up, k, z, x))
        one_down = copy_to(core.at[over, :, pl.ds(128, 128)], first.at[1], (down, k, z, x))
        for there in (up, down, y):
            core[there] += mine[there, k]
        yield
        one_up.wait_recv()
        core[up, :, 0:128] += first[0]
        two_up = copy_to(core.at[up], second.at[0], (up, k, z, x))
        one_down.wait_recv()
        core[down, :, 128:256] += first[1]
        two_down = copy_to(core.at[down], second.at[1], (down, k, z, x))
        yield
        two_up.wait_recv()
        two_down.wait_recv()
        for group in range(group_count):
            value = core[y, group] + second[0, group] + second[1, group]
            home[:, group] = value.reshape(32, 8, 128)

    def share_rows(everyone, home):
        sems = to_columns(lambda there: home.at[there], lambda here: everyone.at[r, here])
        everyone[r, c] = home[c]
        yield
        both = bulk(home.at[pl.ds(0, 31)], everyone.at[r, pl.ds(0, 31)], sems)
        both.wait_recv()
        pending.append(both)
        below, above, beyond = down * 2 + k, up * 2 + k, over * 2 + k
        to_up = copy_to(everyone.at[r], everyone.at[r], (up, k, z, x))
        to_down = copy_to(everyone.at[r], everyone.at[r], (down, k, z, x))
        across = [copy_to(everyone.at[r], everyone.at[r], (y, 1 - k, z, x))]
        yield
        lower, upper = pl.ds(0, 16), pl.ds(16, 16)
        to_up.wait_recv()
        on_up = copy_to(everyone.at[below, lower], everyone.at[below, lower], (up, k, z, x))
        across.append(copy_to(everyone.at[below], everyone.at[below], (y, 1 - k, z, x)))
        to_down.wait_recv()
        on_down = copy_to(everyone.at[above, upper], everyone.at[above, upper], (down, k, z, x))
        across.append(copy_to(everyone.at[above], everyone.at[above], (y, 1 - k, z, x)))
        yield
        on_up.wait_recv()
        on_down.wait_recv()
        across.append(copy_to(everyone.at[beyond], everyone.at[beyond], (y, 1 - k, z, x)))
        yield
        for copy in across:
            copy.wait_recv()

    def ring(size, me, device, chunk, part_of):
        ahead, behind = (me + 1) % size, (me + size - 1) % size
        forth = copy_to(chunk(me), chunk(me), device(ahead))
        back = copy_to(chunk(me), chunk(me), device(behind))
        yield
        for step in range(1, size // 2):
            last = step == size // 2 - 1
            got_low, got_high = (me + size - step) % size, (me + step) % size
            forth.wait_recv()
            low = part_of(got_low, 0) if last else chunk(got_low)
            forth = copy_to(low, low, device(ahead))
            back.wait_recv()
            high = part_of(got_high, 1) if last else chunk(got_high)
            back = copy_to(high, high, device(behind))
            yield
        forth.wait_recv()
        back.wait_recv()

    def chained(*generators):
        for generator in generators:
            yield from generator()

    def run_together(*generators):
        live = list(generators)
        while live:
            for generator in list(live):
                try:
                    next(generator)
                except StopIteration:
                    live.remove(generator)

    lane64 = lax.broadcasted_iota(jnp.int32, (64, 128), 1) < 64
    lane8 = lax.broadcasted_iota(jnp.int32, (8, 128), 1) < 64

    def gather_left(everyone, group):
        for pair in range(16):
            even = everyone[:, 2 * pair, group].reshape(64, 128)
            odd = everyone[:, 2 * pair + 1, group].reshape(64, 128)
            cols = pl.ds(pair * 128, 128)
            for side, value in (
                (0, jnp.where(lane64, even, pltpu.roll(odd, 64, 1))),
                (1, jnp.where(lane64, pltpu.roll(even, 64, 1), odd)),
            ):
                high, low = halves(value)
                l_high[side, 0:64, cols] = high
                l_low[side, 0:64, cols] = low

    def gather_sums(everyone, group):
        for pair in range(16):
            even = jnp.sum(everyone[:, 2 * pair, group], axis=0)
            odd = jnp.sum(everyone[:, 2 * pair + 1, group], axis=0)
            cols = pl.ds(pair * 128, 128)
            blank = jnp.zeros((8, 128), F32)
            for side, value in (
                (0, jnp.where(lane8, even, pltpu.roll(odd, 64, 1))),
                (1, jnp.where(lane8, pltpu.roll(even, 64, 1), odd)),
            ):
                high, low = halves(jnp.concatenate([value, blank], axis=0))
                x_high[side, :, cols] = high
                x_low[side, :, cols] = low

    def times_d(sup, side, with_sums):
        highs, lows = l_high[side], l_low[side]
        if with_sums:
            highs = jnp.concatenate([highs, x_high[side]], axis=0)
            lows = jnp.concatenate([lows, x_low[side]], axis=0)
        value = mm(highs, d_high[sup]) + mm(lows, d_high[sup]) + mm(highs, d_low[sup])
        top = value[0:64]
        own_var[sup, :] = own_var[sup, :] + jnp.sum(top * top, axis=0)
        return value

    def put_mean(sup, rows):
        place = PLACE[sup][1]
        mean_out[sup] = rows[2 * place : 2 * place + 2]

    load1.wait()
    own_var[...] = jnp.zeros_like(own_var)
    round1 = reduce_rows(2, part1, core1, first1, second1, home1)
    next(round1)
    post_all[c] = post[...]
    post_sems = to_columns(lambda there: post, lambda here: post_all.at[here])
    next(round1)

    row_of = lax.broadcasted_iota(jnp.int32, (256, 256), 0)
    col_of = lax.broadcasted_iota(jnp.int32, (256, 256), 1) + r * 256

    def split_d(sup, load):
        load.wait()

        def one(piece, total):
            rows = pl.ds(pl.multiple_of(piece * 256, 256), 256)
            value = jnp.where(row_of + piece * 256 >= col_of, d_raw[sup, rows, :], 0.0)
            high, low = halves(value)
            d_high[sup, rows, :] = high
            d_low[sup, rows, :] = low
            return total + jnp.sum(value * value, axis=0, keepdims=True)

        total = lax.fori_loop(0, 8, one, jnp.zeros((1, 256), F32))
        sums[sup, :] = total[0]

    split_d(*d_loads[0])
    split_d(*d_loads[1])
    next(round1)
    split_d(*d_loads[2])
    split_d(*d_loads[3])
    next(round1, None)
    share1 = share_rows(all1, home1)
    next(share1)
    split_d(*d_loads[4])
    split_d(*d_loads[5])
    next(share1)

    post_both = bulk(post_all.at[pl.ds(0, 31)], post_all.at[pl.ds(0, 31)], post_sems)
    post_both.wait_recv()
    pending.append(post_both)
    for sup in range(NS):
        rows = post_all[:, 2 * sup : 2 * sup + 2, :]
        value = jnp.concatenate([rows] * 4, axis=1).reshape(256, 256)
        high, low = halves(value)
        post_high[sup] = high
        post_low[sup] = low
    next(share1)
    pair_of = (lax.broadcasted_iota(jnp.int32, (256, 128), 0) % 8) // 2
    low_lanes = lax.broadcasted_iota(jnp.int32, (256, 128), 1) < 64

    def placed(sup, value):
        side, pair = PLACE[sup]
        here = low_lanes if side == 0 else jnp.logical_not(low_lanes)
        return jnp.where(here & (pair_of == pair), value, 0.0)

    pick_row = lax.broadcasted_iota(jnp.int32, (256, 128), 0)
    pick_col = lax.broadcasted_iota(jnp.int32, (256, 128), 1) % 64 + x * 64
    picker = jnp.where((pick_row == pick_col) & (r == c // 4), 1.0, 0.0).astype(BF16)
    right_sum = jnp.zeros((256, 128), F32)
    for sup in range(NS):
        value = mm(post_high[sup], picker) + mm(post_low[sup], picker)
        right_sum = right_sum + placed(sup, value)

    def minus_post(right_sum, home, group, slots):
        high, low = halves(home[:, group].reshape(256, 128))
        for slot in slots:
            if slot is None:
                continue
            sup, second = slot
            at = jnp.minimum(ancestor_of(parent, sup, second), NS - 1)
            value = mm(post_high[at], high) + mm(post_low[at], high) + mm(post_high[at], low)
            right_sum = right_sum - placed(sup, value)
        return right_sum

    next(share1)
    for group in range(2):
        right_sum = minus_post(right_sum, home1, group, GROUPS[group])
    next(share1, None)
    drain()

    for group in range(2):
        gather_left(all1, group)
        for side in range(2):
            sup = GROUPS[group][side][0]
            solved[sup] = times_d(sup, side, False)

    inner = []
    for sup in (4, 3, 2, 1):
        has_child = functools.reduce(jnp.logical_or, [parent[below] == sup for below in range(sup)])
        inner.append((sup, jnp.logical_and(parent[sup] < NS, has_child).astype(jnp.int32)))
    picks = []
    before = jnp.int32(0)
    for sup, is_inner in inner:
        picks.append((sup, [is_inner * (before == place).astype(jnp.int32) for place in range(2)]))
        before = before + is_inner
    for place in range(2):
        value = jnp.zeros((64, 256), F32)
        for sup, chosen in picks:
            value = value + solved[sup] * chosen[place].astype(F32)
        spread[z, x, place] = value.reshape(8, 8, 256)

    lower, upper = pl.ds(0, 4), pl.ds(4, 4)
    on_z = lambda there: (y, k, there, x)
    on_x = lambda there: (y, k, z, there)
    order_a = chained(
        lambda: ring(8, z, on_z, lambda i: spread.at[i, x, :, lower], lambda i, q: spread.at[i, x, q, lower]),
        lambda: ring(4, x, on_x, lambda i: spread.at[:, i, :, lower], lambda i, q: spread.at[:, i, q, lower]),
    )
    order_b = chained(
        lambda: ring(4, x, on_x, lambda i: spread.at[z, i, :, upper], lambda i, q: spread.at[z, i, q, upper]),
        lambda: ring(8, z, on_z, lambda i: spread.at[i, :, :, upper], lambda i, q: spread.at[i, :, q, upper]),
    )
    run_together(order_a, order_b)
    drain()

    load_b.wait()
    load2.wait()
    sources = ((2, (1, 0)), (3, (0, 1)), (0, (4, 0)), (1, (1, 1)))
    weights = []
    for place in range(2):
        pieces = []
        for sup, (group, side) in sources:
            chosen = jnp.int32(0)
            for inner_sup, flags in picks:
                if inner_sup > sup:
                    chosen = chosen + flags[place] * (parent[sup] == inner_sup).astype(jnp.int32)
            pieces.append(block_buf[group, side] * chosen.astype(F32))
        weights.append(halves(jnp.concatenate(pieces, axis=0)))
    for row_block in range(8):
        total = jnp.zeros((256, 256), F32)
        for place in range(2):
            high, low = halves(spread[:, :, place, row_block].reshape(256, 256))
            w_high, w_low = weights[place]
            total = total + mm(high, w_high, NT) + mm(low, w_high, NT) + mm(high, w_low, NT)
        at = (row_block // 2, row_block % 2)
        part2[at[0], at[1], 0] = part2[at[0], at[1], 0] - total[:, :128]
        part2[at[0], at[1], 1] = part2[at[0], at[1], 1] - total[:, 128:]

    for _ in reduce_rows(3, part2, core2, first2, second2, home2):
        pass
    for group in range(3):
        right_sum = minus_post(right_sum, home2, group, GROUPS[group + 2])
    home2[:, 3] = right_sum.reshape(32, 8, 128)
    for _ in share_rows(all2, home2):
        pass
    drain()

    gather_sums(all2, 3)
    for group in range(3):
        gather_left(all2, group)
        for side in range(2):
            slot = GROUPS[group + 2][side]
            if slot is None:
                continue
            value = times_d(slot[0], side, group < 2)
            if group < 2:
                put_mean(slot[0], value[64:80])
    for sup in (4, 5):
        side = PLACE[sup][0]
        highs, lows = x_high[side], x_low[side]
        put_mean(sup, mm(highs, d_high[sup]) + mm(lows, d_high[sup]) + mm(highs, d_low[sup]))

    copies = []
    for step in range(1, 4):
        copies.append(copy_to(own_var, sums_x.at[step - 1], (y, k, z, (x + step) % 4)))
    for copy in copies:
        copy.wait_recv()
    sums_z[0] = own_var[...] + sums_x[0] + sums_x[1] + sums_x[2]
    copies = []
    for step in range(1, 8):
        copies.append(copy_to(sums_z.at[0], sums_z.at[step], (y, k, (z + step) % 8, x)))
    for copy in copies:
        copy.wait_recv()
    total = sums[...]
    for step in range(8):
        total = total + sums_z[step]
    var_out[...] = total[0:NS]
    drain()


def sweep(parent, part, blocks, diag_inv, post):
    any_ = pl.BlockSpec(memory_space=pl.ANY)
    vmem = pl.BlockSpec(memory_space=pltpu.VMEM)
    smem = pl.BlockSpec(memory_space=pltpu.SMEM)
    return pl.pallas_call(
        sweep_kernel,
        out_shape=(jax.ShapeDtypeStruct((NS, 2, 256), F32), jax.ShapeDtypeStruct((NS, 256), F32)),
        in_specs=[smem, any_, any_, any_, vmem],
        out_specs=(vmem, vmem),
        scratch_shapes=[
            pltpu.VMEM((4, 2, 2, 256, 128), F32),
            pltpu.VMEM((4, 2, 3, 256, 128), F32),
            pltpu.VMEM((4, 2, 256, 128), F32),
            pltpu.VMEM((4, 3, 256, 128), F32),
            pltpu.VMEM((2, 2, 128, 128), F32),
            pltpu.VMEM((2, 3, 128, 128), F32),
            pltpu.VMEM((2, 2, 256, 128), F32),
            pltpu.VMEM((2, 3, 256, 128), F32),
            pltpu.VMEM((32, 2, 8, 128), F32),
            pltpu.VMEM((32, 4, 8, 128), F32),
            pltpu.VMEM((8, 32, 2, 8, 128), F32),
            pltpu.VMEM((8, 32, 4, 8, 128), F32),
            pltpu.VMEM((8, 4, 2, 8, 8, 256), F32),
            pltpu.VMEM((NS, 2048, 256), F32),
            pltpu.VMEM((NS, 2048, 256), BF16),
            pltpu.VMEM((NS, 2048, 256), BF16),
            pltpu.VMEM((32, 16, 256), F32),
            pltpu.VMEM((NS, 256, 256), BF16),
            pltpu.VMEM((NS, 256, 256), BF16),
            pltpu.VMEM((2, 64, 2048), BF16),
            pltpu.VMEM((2, 64, 2048), BF16),
            pltpu.VMEM((2, 16, 2048), BF16),
            pltpu.VMEM((2, 16, 2048), BF16),
            pltpu.VMEM((5, 64, 256), F32),
            pltpu.VMEM((5, 2, 64, 256), F32),
            pltpu.VMEM((8, 256), F32),
            pltpu.VMEM((3, 8, 256), F32),
            pltpu.VMEM((8, 8, 256), F32),
            pltpu.VMEM((8, 256), F32),
            pltpu.SemaphoreType.DMA((96,)),
            pltpu.SemaphoreType.DMA((96,)),
            pltpu.SemaphoreType.DMA((9,)),
        ],
        compiler_params=pltpu.CompilerParams(
            collective_id=0, has_side_effects=True, vmem_limit_bytes=66_000_000
        ),
        cost_estimate=pl.CostEstimate(flops=8_000_000_000, bytes_accessed=30_000_000, transcendentals=0),
    )(parent, part, blocks, diag_inv, post)


def body(factor, diag_inv, structure, parent, post):
    marks = jnp.transpose(structure, (0, 2, 1))
    blocks = jnp.transpose(factor, (0, 2, 3, 1))
    post_rows = jnp.pad(jnp.transpose(post, (0, 2, 1)).reshape(12, 256), ((0, 4), (0, 0)))
    part, kept = local_products(parent, marks, diag_inv, blocks)
    mean, variance = sweep(parent, part, kept, diag_inv, post_rows)
    return jnp.transpose(mean, (0, 2, 1)), variance


def solution(mesh):
    finer = Mesh(mesh.devices.reshape(4, 2, 8, 4), ("y", "core", "z", "x"))
    row, col = ("y", "core"), ("z", "x")
    placed = (
        P(None, row, None, col),
        P(None, None, row),
        P(None, None, row),
        P(),
        P(None, row, col),
    )
    return jax.shard_map(
        body,
        mesh=finer,
        in_specs=placed,
        out_specs=(P(None, row, col), P(None, row)),
        check_vma=False,
    )
```

```python
import functools

import jax
import jax.numpy as jnp
from jax import lax
from jax.experimental import pallas as pl
from jax.experimental.pallas import tpu as pltpu
from jax.sharding import Mesh
from jax.sharding import PartitionSpec as P

NS = 6
MESH = pl.DeviceIdType.MESH
F32 = jnp.float32
BF16 = jnp.bfloat16
FIRST = (((4, 0), None), ((2, 0), (3, 0)), ((0, 0), (1, 0)))
SECOND = (((2, 1), (3, 1)), ((0, 1), (1, 1)))
PLACE = {4: (0, 0), 2: (0, 1), 0: (0, 2), 3: (1, 0), 1: (1, 1), 5: (1, 2)}
NT = (((1,), (1,)), ((), ()))
NN = (((1,), (0,)), ((), ()))


def halves(value):
    high = value.astype(BF16)
    return high, (value - high.astype(F32)).astype(BF16)


def mm(left, right, dims=NN):
    return lax.dot_general(left, right, dims, preferred_element_type=F32)


def mm3(left, right, dims=NN):
    return mm(left[0], right[0], dims) + mm(left[1], right[0], dims) + mm(left[0], right[1], dims)


def ancestor_of(parent, sup, second):
    first = parent[sup]
    if not second:
        return first
    return jnp.where(first < NS, parent[jnp.minimum(first, NS - 1)], NS)


def inner_flags(parent):
    flags = {}
    for sup in (4, 3, 2, 1):
        has_child = functools.reduce(jnp.logical_or, [parent[below] == sup for below in range(sup)])
        flags[sup] = jnp.logical_and(parent[sup] < NS, has_child).astype(jnp.int32)
    return flags


class Sems:
    def __init__(self, ref):
        self.ref, self.used = ref, 0

    def take(self):
        self.used += 1
        return self.ref.at[self.used - 1]


def sweep_kernel(
    width, parent, marks, blocks, diag_inv, post, mean_out, var_out,
    part1, part2, core1, core2, once1, once2, twice1, twice2, home1, home2, all1, all2, all_up,
    spread, d_raw, d_high, d_low, block_buf, post_all, post_high, post_low, l_high, l_low,
    x_high, x_low, h_high, h_low, own_var, sums, sums_x, sums_z, sends, recvs, locals_,
):
    y, k = lax.axis_index("y"), lax.axis_index("core")
    z, x = lax.axis_index("z"), lax.axis_index("x")
    r, c = y * 2 + k, z * 4 + x
    up, down, over = (y + 1) % 4, (y + 3) % 4, (y + 2) % 4
    send_sems, recv_sems = Sems(sends), Sems(recvs)
    pending = []

    def copy_to(src, dst, device):
        copy = pltpu.make_async_remote_copy(
            src_ref=src, dst_ref=dst, send_sem=send_sems.take(), recv_sem=recv_sems.take(),
            device_id=device, device_id_type=MESH,
        )
        copy.start()
        pending.append(copy)
        return copy

    load_b = pltpu.make_async_copy(blocks, block_buf, locals_.at[6])
    load_b.start()
    d_order = (5, 4, 3, 2, 1, 0)

    def load_d(order):
        load = pltpu.make_async_copy(diag_inv.at[d_order[order]], d_raw.at[order % 3], locals_.at[order])
        load.start()
        return load

    d_loads = [load_d(order) for order in range(3)]

    barrier = pltpu.get_barrier_semaphore()

    def greet(step, carry):
        there = (c + step) % 32
        pl.semaphore_signal(barrier, inc=1, device_id=(y, k, there // 4, there % 4), device_id_type=MESH)
        return carry

    lax.fori_loop(1, 32, greet, 0)
    for device in ((up, k, z, x), (down, k, z, x), (y, 1 - k, z, x)):
        pl.semaphore_signal(barrier, inc=1, device_id=device, device_id_type=MESH)

    def to_columns(source, target):
        send_sem, recv_sem = send_sems.take(), recv_sems.take()

        def one(step, carry):
            there = (c + step) % 32
            pltpu.make_async_remote_copy(
                src_ref=source(there), dst_ref=target(c), send_sem=send_sem, recv_sem=recv_sem,
                device_id=(y, k, there // 4, there % 4), device_id_type=MESH,
            ).start()
            return carry

        lax.fori_loop(1, 32, one, 0)
        return send_sem, recv_sem

    def bulk(sources, target, sems):
        return pltpu.make_async_remote_copy(
            src_ref=sources, dst_ref=target, send_sem=sems[0], recv_sem=sems[1],
            device_id=(y, k, z, (x + 1) % 4), device_id_type=MESH,
        )

    def reduce_rows(part, core, once, twice, home, group):
        swaps = {}
        for name, there in (("over", over), ("up", up), ("down", down), ("own", y)):
            swaps[name] = copy_to(part.at[group, there, 1 - k], core.at[group, there], (y, 1 - k, z, x))
        yield
        swaps["over"].wait_recv()
        core[group, over] += part[group, over, k]
        one_up = copy_to(core.at[group, over, pl.ds(0, 128)], once.at[group, 0], (up, k, z, x))
        one_down = copy_to(core.at[group, over, pl.ds(128, 128)], once.at[group, 1], (down, k, z, x))
        for name, there in (("up", up), ("down", down), ("own", y)):
            swaps[name].wait_recv()
            core[group, there] += part[group, there, k]
        yield
        one_up.wait_recv()
        core[group, up, 0:128] += once[group, 0]
        two_up = copy_to(core.at[group, up], twice.at[group, 0], (up, k, z, x))
        one_down.wait_recv()
        core[group, down, 128:256] += once[group, 1]
        two_down = copy_to(core.at[group, down], twice.at[group, 1], (down, k, z, x))
        yield
        two_up.wait_recv()
        two_down.wait_recv()
        value = core[group, y] + twice[group, 0] + twice[group, 1]
        home[:, group] = value.reshape(32, 8, 128)

    def over_rows(everyone):
        below, above, beyond = down * 2 + k, up * 2 + k, over * 2 + k
        to_up = copy_to(everyone.at[r], everyone.at[r], (up, k, z, x))
        to_down = copy_to(everyone.at[r], everyone.at[r], (down, k, z, x))
        across = [copy_to(everyone.at[r], everyone.at[r], (y, 1 - k, z, x))]
        yield
        lower, upper = pl.ds(0, 16), pl.ds(16, 16)
        to_up.wait_recv()
        on_up = copy_to(everyone.at[below, lower], everyone.at[below, lower], (up, k, z, x))
        across.append(copy_to(everyone.at[below], everyone.at[below], (y, 1 - k, z, x)))
        to_down.wait_recv()
        on_down = copy_to(everyone.at[above, upper], everyone.at[above, upper], (down, k, z, x))
        across.append(copy_to(everyone.at[above], everyone.at[above], (y, 1 - k, z, x)))
        yield
        on_up.wait_recv()
        on_down.wait_recv()
        across.append(copy_to(everyone.at[beyond], everyone.at[beyond], (y, 1 - k, z, x)))
        yield
        for copy in across:
            copy.wait_recv()

    def share_rows(everyone, home):
        sems = to_columns(lambda there: home.at[there], lambda here: everyone.at[r, here])
        everyone[r, c] = home[c]
        yield
        both = bulk(home.at[pl.ds(0, 31)], everyone.at[r, pl.ds(0, 31)], sems)
        both.wait_recv()
        pending.append(both)
        yield from over_rows(everyone)

    def ring(size, me, device, chunk):
        ahead, behind = (me + 1) % size, (me + size - 1) % size
        forth = [copy_to(chunk(me, q), chunk(me, q), device(ahead)) for q in range(2)]
        back = [copy_to(chunk(me, q), chunk(me, q), device(behind)) for q in (1, 0)][::-1]
        yield
        for step in range(1, size // 2):
            last = step == size // 2 - 1
            got_low, got_high = (me + size - step) % size, (me + step) % size
            for q in range(2):
                forth[q].wait_recv()
                if not last or q == 0:
                    low = chunk(got_low, q)
                    forth[q] = copy_to(low, low, device(ahead))
                back[1 - q].wait_recv()
                if not last or q == 0:
                    high = chunk(got_high, 1 - q)
                    back[1 - q] = copy_to(high, high, device(behind))
            yield
        forth[0].wait_recv()
        back[1].wait_recv()

    def chained(*generators):
        for generator in generators:
            yield from generator()

    def run_together(*generators):
        live = list(generators)
        while live:
            for generator in list(live):
                try:
                    next(generator)
                except StopIteration:
                    live.remove(generator)

    row_of = lax.broadcasted_iota(jnp.int32, (256, 256), 0)
    col_of = lax.broadcasted_iota(jnp.int32, (256, 256), 1) + r * 256

    def split_d(order):
        sup = d_order[order]
        d_loads[order].wait()

        def one(piece, total):
            rows = pl.ds(pl.multiple_of(piece * 256, 256), 256)
            value = jnp.where(row_of + piece * 256 >= col_of, d_raw[order % 3, rows, :], 0.0)
            high, low = halves(value)
            d_high[sup, rows, :] = high
            d_low[sup, rows, :] = low
            return total + jnp.sum(value * value, axis=0, keepdims=True)

        total = lax.fori_loop(0, 8, one, jnp.zeros((1, 256), F32))
        sums[sup, :] = total[0]
        if order + 3 < NS:
            d_loads.append(load_d(order + 3))

    for order in range(5):
        split_d(order)
    load_b.wait()

    row_lane = lax.broadcasted_iota(jnp.int32, (64, 256), 1)

    def multiply(part, group, slots):
        nothing = jnp.zeros((64, 256), BF16)
        terms = []
        for side, slot in enumerate(slots):
            if slot is None:
                continue
            sup, second = slot
            target = ancestor_of(parent, sup, second)
            valid = target < NS
            at = jnp.minimum(target, NS - 1)
            upper_mark = jnp.where(valid, marks[sup, 0, at], 0).astype(F32)
            lower_mark = jnp.where(valid, marks[sup, 1, at], 0).astype(F32)
            block = block_buf[at, sup] * jnp.where(row_lane < 128, upper_mark, lower_mark)
            high, low = halves(block)
            if side == 0:
                both, one = [high, nothing, low, nothing], [high, nothing, nothing, nothing]
            else:
                both, one = [nothing, high, nothing, low], [nothing, high, nothing, nothing]
            terms.append((at, jnp.concatenate(both, axis=0), jnp.concatenate(one, axis=0)))
        for piece in range(8):
            rows = pl.ds(piece * 256, 256)
            total = jnp.zeros((256, 256), F32)
            for at, both, one in terms:
                total = total + mm(d_high[at, rows, :], both, NT) + mm(d_low[at, rows, :], one, NT)
            part[group, piece // 2, piece % 2] = total[:, :128] + total[:, 128:]

    sums1 = [reduce_rows(part1, core1, once1, twice1, home1, group) for group in range(3)]
    sums2 = [reduce_rows(part2, core2, once2, twice2, home2, group) for group in range(2)]
    own_var[...] = jnp.zeros_like(own_var)
    multiply(part1, 0, FIRST[0])
    pl.semaphore_wait(barrier, 34)
    next(sums1[0])
    post_all[c] = post[...]
    post_sems = to_columns(lambda there: post, lambda here: post_all.at[here])
    multiply(part1, 1, FIRST[1])
    next(sums1[1])
    next(sums1[0])
    multiply(part1, 2, FIRST[2])
    next(sums1[2])
    next(sums1[1])
    next(sums1[0])
    multiply(part2, 0, SECOND[0])
    next(sums1[2])
    next(sums1[1])
    multiply(part2, 1, SECOND[1])
    next(sums1[2])
    next(sums1[0], None)
    split_d(5)
    next(sums1[1], None)
    next(sums2[0])
    next(sums2[1])
    next(sums1[2], None)

    flags = inner_flags(parent)
    picks = []
    before = jnp.int32(0)
    for sup in (4, 3, 2, 1):
        picks.append((sup, [flags[sup] * (before == place).astype(jnp.int32) for place in range(width)]))
        before = before + flags[sup]
    where_of = {4: (0, 0), 2: (1, 0), 3: (1, 1), 1: (2, 1)}
    low_lanes = lax.broadcasted_iota(jnp.int32, (256, 128), 1) < 64
    firsts = [home1[:, tile].reshape(256, 128) for tile in range(3)]
    chosen = []
    for place in range(width):
        sides = [jnp.zeros((256, 128), F32), jnp.zeros((256, 128), F32)]
        for sup, weight in picks:
            tile, side = where_of[sup]
            sides[side] = sides[side] + firsts[tile] * weight[place].astype(F32)
        chosen.append(sides)
    rolled = lambda value: pltpu.roll(value, 64, 1)
    if width == 1:
        lo, hi = chosen[0]
        in_low = jnp.where(low_lanes, lo + rolled(hi), 0.0)
        spread[z, x] = jnp.where(low_lanes[0:128], in_low[0:128], rolled(in_low[128:256]))
    else:
        lo = chosen[0][0] + rolled(chosen[0][1])
        hi = rolled(chosen[1][0]) + chosen[1][1]
        spread[z, x] = jnp.where(low_lanes, lo, hi)

    size = width * 128
    quarter = size // 4
    on_z = lambda there: (y, k, there, x)
    on_x = lambda there: (y, k, z, there)
    quarter_of = lambda part_at: pl.ds(part_at * quarter, quarter)
    order_a = chained(
        lambda: ring(8, z, on_z, lambda i, q: spread.at[i, x, quarter_of(q)]),
        lambda: ring(4, x, on_x, lambda i, q: spread.at[:, i, quarter_of(q)]),
    )
    order_b = chained(
        lambda: ring(4, x, on_x, lambda i, q: spread.at[z, i, quarter_of(2 + q)]),
        lambda: ring(8, z, on_z, lambda i, q: spread.at[i, :, quarter_of(2 + q)]),
    )

    def up_copies():
        all_up[r] = home1[:, 1:3]
        yield from over_rows(all_up)

    pair_of = (lax.broadcasted_iota(jnp.int32, (256, 128), 0) % 8) // 2

    def placed(sup, value):
        side, pair = PLACE[sup]
        here = low_lanes if side == 0 else jnp.logical_not(low_lanes)
        return jnp.where(here & (pair_of == pair), value, 0.0)

    right_sum = [jnp.zeros((256, 128), F32)]

    def minus_post(home, group, slots):
        parts = halves(home[:, group].reshape(256, 128))
        for slot in slots:
            if slot is None:
                continue
            sup, second = slot
            at = jnp.minimum(ancestor_of(parent, sup, second), NS - 1)
            value = mm3((post_high[at], post_low[at]), parts)
            right_sum[0] = right_sum[0] - placed(sup, value)

    def right_sides():
        yield
        post_both = bulk(post_all.at[pl.ds(0, 31)], post_all.at[pl.ds(0, 31)], post_sems)
        post_both.wait_recv()
        pending.append(post_both)
        for sup in range(NS):
            rows = post_all[:, 2 * sup : 2 * sup + 2, :]
            value = jnp.concatenate([rows] * 4, axis=1).reshape(256, 256)
            high, low = halves(value)
            post_high[sup] = high
            post_low[sup] = low
        yield
        pick_row = lax.broadcasted_iota(jnp.int32, (256, 128), 0)
        pick_col = lax.broadcasted_iota(jnp.int32, (256, 128), 1) % 64 + x * 64
        picker = jnp.where((pick_row == pick_col) & (r == c // 4), 1.0, 0.0).astype(BF16)
        for sup in range(NS):
            value = mm(post_high[sup], picker) + mm(post_low[sup], picker)
            right_sum[0] = right_sum[0] + placed(sup, value)
        yield
        for group in range(3):
            minus_post(home1, group, FIRST[group])

    share1 = share_rows(all1, home1)
    run_together(
        order_a,
        order_b,
        chained(lambda: up_copies(), lambda: sums2[0]),
        sums2[1],
        right_sides(),
    )

    next(share1)
    for pair in range(16):
        cols = pl.ds(pair * 128, 128)
        even = spread[pair // 2, 2 * (pair % 2)]
        odd = spread[pair // 2, 2 * (pair % 2) + 1]
        wide = low_lanes[0:size]
        for side, value in (
            (0, jnp.where(wide, even, rolled(odd))),
            (1, jnp.where(wide, rolled(even), odd)),
        ):
            high, low = halves(value)
            rows = pl.ds(side * size, size)
            h_high[rows, cols] = high
            h_low[rows, cols] = low
    lane_256 = lax.broadcasted_iota(jnp.int32, (1, 256), 1)
    through = jnp.zeros((256, 256), F32)
    for place in range(width):
        keep = jnp.zeros((1, 256), F32)
        for at, sup in enumerate((2, 3, 0, 1)):
            chosen_here = jnp.int32(0)
            for inner_sup, weight in picks:
                if inner_sup > sup:
                    chosen_here = chosen_here + weight[place] * (parent[sup] == inner_sup).astype(jnp.int32)
            keep = keep + jnp.where(lane_256 // 64 == at, chosen_here.astype(F32), 0.0)
        for row_block in range(8):
            right = jnp.concatenate(
                [all_up[row_block, :, tile].reshape(256, 128) for tile in range(2)], axis=1
            )
            cols = pl.ds(row_block * 256, 256)
            rows = pl.ds(place * 256, 256)
            through = through + mm3((h_high[rows, cols], h_low[rows, cols]), halves(right * keep))
    for group in range(2):
        value = home2[:, group].reshape(256, 128) - through[:, group * 128 : group * 128 + 128]
        home2[:, group] = value.reshape(32, 8, 128)
    for group in range(2):
        minus_post(home2, group, SECOND[group])
    home2[:, 2] = right_sum[0].reshape(32, 8, 128)

    lane64 = low_lanes[0:64]
    lane8 = low_lanes[0:8]

    def gather_left(everyone, group):
        for pair in range(16):
            even = everyone[:, 2 * pair, group].reshape(64, 128)
            odd = everyone[:, 2 * pair + 1, group].reshape(64, 128)
            cols = pl.ds(pair * 128, 128)
            for side, value in (
                (0, jnp.where(lane64, even, rolled(odd))),
                (1, jnp.where(lane64, rolled(even), odd)),
            ):
                high, low = halves(value)
                l_high[side, 0:64, cols] = high
                l_low[side, 0:64, cols] = low

    def gather_sums(everyone, group):
        for pair in range(16):
            even = jnp.sum(everyone[:, 2 * pair, group], axis=0)
            odd = jnp.sum(everyone[:, 2 * pair + 1, group], axis=0)
            cols = pl.ds(pair * 128, 128)
            blank = jnp.zeros((8, 128), F32)
            for side, value in (
                (0, jnp.where(lane8, even, rolled(odd))),
                (1, jnp.where(lane8, rolled(even), odd)),
            ):
                high, low = halves(jnp.concatenate([value, blank], axis=0))
                x_high[side, :, cols] = high
                x_low[side, :, cols] = low

    def times_d(sup, side, with_sums):
        highs, lows = l_high[side], l_low[side]
        if with_sums:
            highs = jnp.concatenate([highs, x_high[side]], axis=0)
            lows = jnp.concatenate([lows, x_low[side]], axis=0)
        value = mm3((highs, lows), (d_high[sup], d_low[sup]))
        top = value[0:64]
        own_var[sup, :] = own_var[sup, :] + jnp.sum(top * top, axis=0)
        return value

    def put_mean(sup, rows):
        place = PLACE[sup][1]
        mean_out[sup] = rows[2 * place : 2 * place + 2]

    def products(everyone, group, slots, with_sums):
        gather_left(everyone, group)
        for side, slot in enumerate(slots):
            if slot is None:
                continue
            value = times_d(slot[0], side, with_sums)
            if with_sums:
                put_mean(slot[0], value[64:80])

    share2 = share_rows(all2, home2)
    next(share2)
    next(share1)
    next(share1)
    next(share2)
    next(share1)
    next(share1, None)
    next(share2)
    for group in range(3):
        products(all1, group, FIRST[group], False)
    next(share2)
    next(share2, None)
    gather_sums(all2, 2)
    for group in range(2):
        products(all2, group, SECOND[group], True)
    for sup in (4, 5):
        side = PLACE[sup][0]
        put_mean(sup, mm3((x_high[side], x_low[side]), (d_high[sup], d_low[sup])))

    copies = []
    for step in range(1, 4):
        copies.append(copy_to(own_var, sums_x.at[step - 1], (y, k, z, (x + step) % 4)))
    for copy in copies:
        copy.wait_recv()
    sums_z[0] = own_var[...] + sums_x[0] + sums_x[1] + sums_x[2]
    copies = []
    for step in range(1, 8):
        copies.append(copy_to(sums_z.at[0], sums_z.at[step], (y, k, (z + step) % 8, x)))
    for copy in copies:
        copy.wait_recv()
    total = sums[...]
    for step in range(8):
        total = total + sums_z[step]
    var_out[...] = total[0:NS]
    while pending:
        pending.pop().wait_send()


def sweep(width, parent, marks, blocks, diag_inv, post):
    any_ = pl.BlockSpec(memory_space=pl.ANY)
    vmem = pl.BlockSpec(memory_space=pltpu.VMEM)
    smem = pl.BlockSpec(memory_space=pltpu.SMEM)
    return pl.pallas_call(
        functools.partial(sweep_kernel, width),
        out_shape=(jax.ShapeDtypeStruct((NS, 2, 256), F32), jax.ShapeDtypeStruct((NS, 256), F32)),
        in_specs=[smem, smem, any_, any_, vmem],
        out_specs=(vmem, vmem),
        scratch_shapes=[
            pltpu.VMEM((3, 4, 2, 256, 128), F32),
            pltpu.VMEM((2, 4, 2, 256, 128), F32),
            pltpu.VMEM((3, 4, 256, 128), F32),
            pltpu.VMEM((2, 4, 256, 128), F32),
            pltpu.VMEM((3, 2, 128, 128), F32),
            pltpu.VMEM((2, 2, 128, 128), F32),
            pltpu.VMEM((3, 2, 256, 128), F32),
            pltpu.VMEM((2, 2, 256, 128), F32),
            pltpu.VMEM((32, 3, 8, 128), F32),
            pltpu.VMEM((32, 3, 8, 128), F32),
            pltpu.VMEM((8, 32, 3, 8, 128), F32),
            pltpu.VMEM((8, 32, 3, 8, 128), F32),
            pltpu.VMEM((8, 32, 2, 8, 128), F32),
            pltpu.VMEM((8, 4, width * 128, 128), F32),
            pltpu.VMEM((3, 2048, 256), F32),
            pltpu.VMEM((NS, 2048, 256), BF16),
            pltpu.VMEM((NS, 2048, 256), BF16),
            pltpu.VMEM((NS, NS, 64, 256), F32),
            pltpu.VMEM((32, 16, 256), F32),
            pltpu.VMEM((NS, 256, 256), BF16),
            pltpu.VMEM((NS, 256, 256), BF16),
            pltpu.VMEM((2, 64, 2048), BF16),
            pltpu.VMEM((2, 64, 2048), BF16),
            pltpu.VMEM((2, 16, 2048), BF16),
            pltpu.VMEM((2, 16, 2048), BF16),
            pltpu.VMEM((width * 256, 2048), BF16),
            pltpu.VMEM((width * 256, 2048), BF16),
            pltpu.VMEM((8, 256), F32),
            pltpu.VMEM((8, 256), F32),
            pltpu.VMEM((3, 8, 256), F32),
            pltpu.VMEM((8, 8, 256), F32),
            pltpu.SemaphoreType.DMA((160,)),
            pltpu.SemaphoreType.DMA((160,)),
            pltpu.SemaphoreType.DMA((7,)),
        ],
        compiler_params=pltpu.CompilerParams(
            collective_id=width - 1, has_side_effects=True, vmem_limit_bytes=67_000_000
        ),
        cost_estimate=pl.CostEstimate(flops=12_000_000_000, bytes_accessed=30_000_000, transcendentals=0),
    )(parent, marks, blocks, diag_inv, post)


def body(factor, diag_inv, structure, parent, post):
    marks = jnp.transpose(structure, (0, 2, 1))
    blocks = jnp.transpose(factor, (0, 2, 3, 1))
    post_rows = jnp.pad(jnp.transpose(post, (0, 2, 1)).reshape(12, 256), ((0, 4), (0, 0)))
    mean, variance = sweep(2, parent, marks, blocks, diag_inv, post_rows)
    return jnp.transpose(mean, (0, 2, 1)), variance


def solution(mesh):
    finer = Mesh(mesh.devices.reshape(4, 2, 8, 4), ("y", "core", "z", "x"))
    row, col = ("y", "core"), ("z", "x")
    placed = (
        P(None, row, None, col),
        P(None, None, row),
        P(None, None, row),
        P(),
        P(None, row, col),
    )
    return jax.shard_map(
        body,
        mesh=finer,
        in_specs=placed,
        out_specs=(P(None, row, col), P(None, row)),
        check_vma=False,
    )
```

```python
import functools

import jax
import jax.numpy as jnp
from jax import lax
from jax.experimental import pallas as pl
from jax.experimental.pallas import tpu as pltpu
from jax.sharding import Mesh
from jax.sharding import PartitionSpec as P

NS = 6
MESH = pl.DeviceIdType.MESH
F32 = jnp.float32
BF16 = jnp.bfloat16
FIRST = (((4, 0), None), ((2, 0), (3, 0)), ((0, 0), (1, 0)))
SECOND = (((2, 1), (3, 1)), ((0, 1), (1, 1)))
PLACE = {4: (0, 0), 2: (0, 1), 0: (0, 2), 3: (1, 0), 1: (1, 1), 5: (1, 2)}
NT = (((1,), (1,)), ((), ()))
NN = (((1,), (0,)), ((), ()))


def halves(value):
    high = value.astype(BF16)
    return high, (value - high.astype(F32)).astype(BF16)


def mm(left, right, dims=NN):
    return lax.dot_general(left, right, dims, preferred_element_type=F32)


def mm3(left, right, dims=NN):
    return mm(left[0], right[0], dims) + mm(left[1], right[0], dims) + mm(left[0], right[1], dims)


def ancestor_of(parent, sup, second):
    first = parent[sup]
    if not second:
        return first
    return jnp.where(first < NS, parent[jnp.minimum(first, NS - 1)], NS)


def inner_flags(parent):
    flags = {}
    for sup in (4, 3, 2, 1):
        has_child = functools.reduce(jnp.logical_or, [parent[below] == sup for below in range(sup)])
        flags[sup] = jnp.logical_and(parent[sup] < NS, has_child).astype(jnp.int32)
    return flags


class Sems:
    def __init__(self, ref):
        self.ref, self.used = ref, 0

    def take(self):
        self.used += 1
        return self.ref.at[self.used - 1]


def sweep_kernel(
    width, parent, marks, blocks, diag_inv, post, mean_out, var_out,
    part1, part2, core1, core2, once1, once2, twice1, twice2, home1, home2, all1, all2, all_up,
    spread, d_raw, d_high, d_low, block_buf, post_all, post_high, post_low, l_high, l_low,
    x_high, x_low, h_high, h_low, post_rows, own_var, sums, sums_x, sums_z, sends, recvs, locals_,
):
    y, k = lax.axis_index("y"), lax.axis_index("core")
    z, x = lax.axis_index("z"), lax.axis_index("x")
    r, c = y * 2 + k, z * 4 + x
    up, down, over = (y + 1) % 4, (y + 3) % 4, (y + 2) % 4
    send_sems, recv_sems = Sems(sends), Sems(recvs)
    pending = []

    def copy_to(src, dst, device):
        copy = pltpu.make_async_remote_copy(
            src_ref=src, dst_ref=dst, send_sem=send_sems.take(), recv_sem=recv_sems.take(),
            device_id=device, device_id_type=MESH,
        )
        copy.start()
        pending.append(copy)
        return copy

    load_b = pltpu.make_async_copy(blocks, block_buf, locals_.at[6])
    load_b.start()
    d_order = (5, 4, 3, 2, 1, 0)

    def load_d(order):
        load = pltpu.make_async_copy(diag_inv.at[d_order[order]], d_raw.at[order % 3], locals_.at[order])
        load.start()
        return load

    d_loads = [load_d(order) for order in range(3)]

    barrier = pltpu.get_barrier_semaphore()

    def greet(step, carry):
        there = (c + step) % 32
        pl.semaphore_signal(barrier, inc=1, device_id=(y, k, there // 4, there % 4), device_id_type=MESH)
        return carry

    lax.fori_loop(1, 32, greet, 0)
    for device in ((up, k, z, x), (down, k, z, x), (y, 1 - k, z, x)):
        pl.semaphore_signal(barrier, inc=1, device_id=device, device_id_type=MESH)

    def to_columns(source, target, sems=None, steps=(1, 32)):
        send_sem, recv_sem = sems or (send_sems.take(), recv_sems.take())

        def one(step, carry):
            there = (c + step) % 32
            pltpu.make_async_remote_copy(
                src_ref=source(there), dst_ref=target(c), send_sem=send_sem, recv_sem=recv_sem,
                device_id=(y, k, there // 4, there % 4), device_id_type=MESH,
            ).start()
            return carry

        lax.fori_loop(*steps, one, 0)
        return send_sem, recv_sem

    def bulk(sources, target, sems):
        return pltpu.make_async_remote_copy(
            src_ref=sources, dst_ref=target, send_sem=sems[0], recv_sem=sems[1],
            device_id=(y, k, z, (x + 1) % 4), device_id_type=MESH,
        )

    def reduce_rows(part, core, once, twice, home, group):
        swaps = {}
        for name, there in (("over", over), ("up", up), ("down", down), ("own", y)):
            swaps[name] = copy_to(part.at[group, there, 1 - k], core.at[group, there], (y, 1 - k, z, x))
        yield
        swaps["over"].wait_recv()
        core[group, over] += part[group, over, k]
        one_up = copy_to(core.at[group, over, pl.ds(0, 128)], once.at[group, 0], (up, k, z, x))
        one_down = copy_to(core.at[group, over, pl.ds(128, 128)], once.at[group, 1], (down, k, z, x))
        for name, there in (("up", up), ("down", down), ("own", y)):
            swaps[name].wait_recv()
            core[group, there] += part[group, there, k]
        yield
        one_up.wait_recv()
        core[group, up, 0:128] += once[group, 0]
        two_up = copy_to(core.at[group, up], twice.at[group, 0], (up, k, z, x))
        one_down.wait_recv()
        core[group, down, 128:256] += once[group, 1]
        two_down = copy_to(core.at[group, down], twice.at[group, 1], (down, k, z, x))
        yield
        two_up.wait_recv()
        two_down.wait_recv()
        value = core[group, y] + twice[group, 0] + twice[group, 1]
        home[:, group] = value.reshape(32, 8, 128)

    def over_rows(everyone):
        below, above, beyond = down * 2 + k, up * 2 + k, over * 2 + k
        to_up = copy_to(everyone.at[r], everyone.at[r], (up, k, z, x))
        to_down = copy_to(everyone.at[r], everyone.at[r], (down, k, z, x))
        across = [copy_to(everyone.at[r], everyone.at[r], (y, 1 - k, z, x))]
        yield
        lower, upper = pl.ds(0, 16), pl.ds(16, 16)
        to_up.wait_recv()
        on_up = copy_to(everyone.at[below, lower], everyone.at[below, lower], (up, k, z, x))
        across.append(copy_to(everyone.at[below], everyone.at[below], (y, 1 - k, z, x)))
        to_down.wait_recv()
        on_down = copy_to(everyone.at[above, upper], everyone.at[above, upper], (down, k, z, x))
        across.append(copy_to(everyone.at[above], everyone.at[above], (y, 1 - k, z, x)))
        yield
        on_up.wait_recv()
        on_down.wait_recv()
        across.append(copy_to(everyone.at[beyond], everyone.at[beyond], (y, 1 - k, z, x)))
        yield
        for copy in across:
            copy.wait_recv()

    def share_rows(everyone, home, pieces=1):
        everyone[r, c] = home[c]
        sems = None
        for piece in range(pieces):
            steps = (1 + 31 * piece // pieces, 1 + 31 * (piece + 1) // pieces)
            sems = to_columns(lambda there: home.at[there], lambda here: everyone.at[r, here], sems, steps)
            yield
        both = bulk(home.at[pl.ds(0, 31)], everyone.at[r, pl.ds(0, 31)], sems)
        both.wait_recv()
        pending.append(both)
        yield from over_rows(everyone)

    def ring(size, me, device, chunk):
        ahead, behind = (me + 1) % size, (me + size - 1) % size
        forth = [copy_to(chunk(me, q), chunk(me, q), device(ahead)) for q in range(2)]
        back = [copy_to(chunk(me, q), chunk(me, q), device(behind)) for q in (1, 0)][::-1]
        yield
        for step in range(1, size // 2):
            last = step == size // 2 - 1
            got_low, got_high = (me + size - step) % size, (me + step) % size
            for q in range(2):
                forth[q].wait_recv()
                if not last or q == 0:
                    low = chunk(got_low, q)
                    forth[q] = copy_to(low, low, device(ahead))
                back[1 - q].wait_recv()
                if not last or q == 0:
                    high = chunk(got_high, 1 - q)
                    back[1 - q] = copy_to(high, high, device(behind))
            yield
        forth[0].wait_recv()
        back[1].wait_recv()

    def chained(*generators):
        for generator in generators:
            yield from generator()

    def run_together(generators, beside):
        live = list(generators)
        while live:
            for generator in list(live):
                if next(generator, "end") == "end":
                    live.remove(generator)
            next(beside, None)

    row_of = lax.broadcasted_iota(jnp.int32, (256, 256), 0)
    col_of = lax.broadcasted_iota(jnp.int32, (256, 256), 1) + r * 256

    def split_d(order):
        sup = d_order[order]
        d_loads[order].wait()

        def one(piece, total):
            rows = pl.ds(pl.multiple_of(piece * 256, 256), 256)
            value = jnp.where(row_of + piece * 256 >= col_of, d_raw[order % 3, rows, :], 0.0)
            high, low = halves(value)
            d_high[sup, rows, :] = high
            d_low[sup, rows, :] = low
            return total + jnp.sum(value * value, axis=0, keepdims=True)

        total = lax.fori_loop(0, 8, one, jnp.zeros((1, 256), F32))
        sums[sup, :] = total[0]
        if order + 3 < NS:
            d_loads.append(load_d(order + 3))

    split_d(0)
    load_b.wait()

    row_lane = lax.broadcasted_iota(jnp.int32, (64, 256), 1)

    def multiply(part, group, slots):
        nothing = jnp.zeros((64, 256), BF16)
        terms = []
        for side, slot in enumerate(slots):
            if slot is None:
                continue
            sup, second = slot
            target = ancestor_of(parent, sup, second)
            valid = target < NS
            at = jnp.minimum(target, NS - 1)
            upper_mark = jnp.where(valid, marks[sup, 0, at], 0).astype(F32)
            lower_mark = jnp.where(valid, marks[sup, 1, at], 0).astype(F32)
            block = block_buf[at, sup] * jnp.where(row_lane < 128, upper_mark, lower_mark)
            high, low = halves(block)
            if side == 0:
                both, one = [high, nothing, low, nothing], [high, nothing, nothing, nothing]
            else:
                both, one = [nothing, high, nothing, low], [nothing, high, nothing, nothing]
            terms.append((at, jnp.concatenate(both, axis=0), jnp.concatenate(one, axis=0)))
        for piece in range(8):
            rows = pl.ds(piece * 256, 256)
            total = jnp.zeros((256, 256), F32)
            for at, both, one in terms:
                total = total + mm(d_high[at, rows, :], both, NT) + mm(d_low[at, rows, :], one, NT)
            part[group, piece // 2, piece % 2] = total[:, :128] + total[:, 128:]

    sums1 = [reduce_rows(part1, core1, once1, twice1, home1, group) for group in range(3)]
    sums2 = [reduce_rows(part2, core2, once2, twice2, home2, group) for group in range(2)]
    own_var[...] = jnp.zeros_like(own_var)
    multiply(part1, 0, FIRST[0])
    for sup in range(NS):
        post_rows[2 * sup : 2 * sup + 2, :] = post[sup]
    post_rows[2 * NS : 16, :] = jnp.zeros((16 - 2 * NS, 256), F32)
    pl.semaphore_wait(barrier, 34)
    next(sums1[0])
    post_all[c] = post_rows[...]
    post_sems = to_columns(lambda there: post_rows, lambda here: post_all.at[here])
    split_d(1)
    next(sums1[0])
    split_d(2)
    multiply(part1, 1, FIRST[1])
    next(sums1[1])
    next(sums1[0])
    split_d(3)
    next(sums1[1])
    split_d(4)
    multiply(part1, 2, FIRST[2])
    next(sums1[2])
    next(sums1[0], None)
    next(sums1[1])
    next(sums1[2])
    multiply(part2, 0, SECOND[0])
    next(sums1[1], None)
    next(sums1[2])
    multiply(part2, 1, SECOND[1])
    next(sums2[0])
    next(sums2[1])
    split_d(5)
    next(sums1[2], None)

    flags = inner_flags(parent)
    picks = []
    before = jnp.int32(0)
    for sup in (4, 3, 2, 1):
        picks.append((sup, [flags[sup] * (before == place).astype(jnp.int32) for place in range(width)]))
        before = before + flags[sup]
    where_of = {4: (0, 0), 2: (1, 0), 3: (1, 1), 1: (2, 1)}
    low_lanes = lax.broadcasted_iota(jnp.int32, (256, 128), 1) < 64
    firsts = [home1[:, tile].reshape(256, 128) for tile in range(3)]
    chosen = []
    for place in range(width):
        sides = [jnp.zeros((256, 128), F32), jnp.zeros((256, 128), F32)]
        for sup, weight in picks:
            tile, side = where_of[sup]
            sides[side] = sides[side] + firsts[tile] * weight[place].astype(F32)
        chosen.append(sides)
    rolled = lambda value: pltpu.roll(value, 64, 1)
    if width == 1:
        lo, hi = chosen[0]
        in_low = jnp.where(low_lanes, lo + rolled(hi), 0.0)
        spread[z, x] = jnp.where(low_lanes[0:128], in_low[0:128], rolled(in_low[128:256]))
    else:
        lo = chosen[0][0] + rolled(chosen[0][1])
        hi = rolled(chosen[1][0]) + chosen[1][1]
        spread[z, x] = jnp.where(low_lanes, lo, hi)

    size = width * 128
    quarter = size // 4
    on_z = lambda there: (y, k, there, x)
    on_x = lambda there: (y, k, z, there)
    quarter_of = lambda part_at: pl.ds(part_at * quarter, quarter)
    order_a = chained(
        lambda: ring(8, z, on_z, lambda i, q: spread.at[i, x, quarter_of(q)]),
        lambda: ring(4, x, on_x, lambda i, q: spread.at[:, i, quarter_of(q)]),
    )
    order_b = chained(
        lambda: ring(4, x, on_x, lambda i, q: spread.at[z, i, quarter_of(2 + q)]),
        lambda: ring(8, z, on_z, lambda i, q: spread.at[i, :, quarter_of(2 + q)]),
    )

    def up_copies():
        all_up[r] = home1[:, 1:3]
        yield from over_rows(all_up)

    pair_of = (lax.broadcasted_iota(jnp.int32, (256, 128), 0) % 8) // 2

    def placed(sup, value):
        side, pair = PLACE[sup]
        here = low_lanes if side == 0 else jnp.logical_not(low_lanes)
        return jnp.where(here & (pair_of == pair), value, 0.0)

    right_sum = [jnp.zeros((256, 128), F32)]

    def minus_post(home, group, slots):
        parts = halves(home[:, group].reshape(256, 128))
        for slot in slots:
            if slot is None:
                continue
            sup, second = slot
            at = jnp.minimum(ancestor_of(parent, sup, second), NS - 1)
            value = mm3((post_high[at], post_low[at]), parts)
            right_sum[0] = right_sum[0] - placed(sup, value)

    def right_sides():
        yield
        post_both = bulk(post_all.at[pl.ds(0, 31)], post_all.at[pl.ds(0, 31)], post_sems)
        post_both.wait_recv()
        pending.append(post_both)
        for sup in range(NS):
            rows = post_all[:, 2 * sup : 2 * sup + 2, :]
            value = jnp.concatenate([rows] * 4, axis=1).reshape(256, 256)
            high, low = halves(value)
            post_high[sup] = high
            post_low[sup] = low
        yield
        pick_row = lax.broadcasted_iota(jnp.int32, (256, 128), 0)
        pick_col = lax.broadcasted_iota(jnp.int32, (256, 128), 1) % 64 + x * 64
        picker = jnp.where((pick_row == pick_col) & (r == c // 4), 1.0, 0.0).astype(BF16)
        for sup in range(NS):
            value = mm(post_high[sup], picker) + mm(post_low[sup], picker)
            right_sum[0] = right_sum[0] + placed(sup, value)
        yield
        for group in range(3):
            minus_post(home1, group, FIRST[group])

    share1 = share_rows(all1, home1, 4)
    run_together((order_a, order_b, sums2[0], sums2[1], up_copies(), right_sides()), share1)

    for pair in range(16):
        cols = pl.ds(pair * 128, 128)
        even = spread[pair // 2, 2 * (pair % 2)]
        odd = spread[pair // 2, 2 * (pair % 2) + 1]
        wide = low_lanes[0:size]
        for side, value in (
            (0, jnp.where(wide, even, rolled(odd))),
            (1, jnp.where(wide, rolled(even), odd)),
        ):
            high, low = halves(value)
            rows = pl.ds(side * size, size)
            h_high[rows, cols] = high
            h_low[rows, cols] = low
    lane_256 = lax.broadcasted_iota(jnp.int32, (1, 256), 1)
    through = jnp.zeros((256, 256), F32)
    for place in range(width):
        keep = jnp.zeros((1, 256), F32)
        for at, sup in enumerate((2, 3, 0, 1)):
            chosen_here = jnp.int32(0)
            for inner_sup, weight in picks:
                if inner_sup > sup:
                    chosen_here = chosen_here + weight[place] * (parent[sup] == inner_sup).astype(jnp.int32)
            keep = keep + jnp.where(lane_256 // 64 == at, chosen_here.astype(F32), 0.0)
        for row_block in range(8):
            right = jnp.concatenate(
                [all_up[row_block, :, tile].reshape(256, 128) for tile in range(2)], axis=1
            )
            cols = pl.ds(row_block * 256, 256)
            rows = pl.ds(place * 256, 256)
            through = through + mm3((h_high[rows, cols], h_low[rows, cols]), halves(right * keep))
    for group in range(2):
        value = home2[:, group].reshape(256, 128) - through[:, group * 128 : group * 128 + 128]
        home2[:, group] = value.reshape(32, 8, 128)
    for group in range(2):
        minus_post(home2, group, SECOND[group])
    home2[:, 2] = right_sum[0].reshape(32, 8, 128)

    lane64 = low_lanes[0:64]
    lane8 = low_lanes[0:8]

    def gather_left(everyone, group):
        for pair in range(16):
            even = everyone[:, 2 * pair, group].reshape(64, 128)
            odd = everyone[:, 2 * pair + 1, group].reshape(64, 128)
            cols = pl.ds(pair * 128, 128)
            for side, value in (
                (0, jnp.where(lane64, even, rolled(odd))),
                (1, jnp.where(lane64, rolled(even), odd)),
            ):
                high, low = halves(value)
                l_high[side, 0:64, cols] = high
                l_low[side, 0:64, cols] = low

    def gather_sums(everyone, group):
        for pair in range(16):
            even = jnp.sum(everyone[:, 2 * pair, group], axis=0)
            odd = jnp.sum(everyone[:, 2 * pair + 1, group], axis=0)
            cols = pl.ds(pair * 128, 128)
            blank = jnp.zeros((8, 128), F32)
            for side, value in (
                (0, jnp.where(lane8, even, rolled(odd))),
                (1, jnp.where(lane8, rolled(even), odd)),
            ):
                high, low = halves(jnp.concatenate([value, blank], axis=0))
                x_high[side, :, cols] = high
                x_low[side, :, cols] = low

    def times_d(sup, side, with_sums):
        highs, lows = l_high[side], l_low[side]
        if with_sums:
            highs = jnp.concatenate([highs, x_high[side]], axis=0)
            lows = jnp.concatenate([lows, x_low[side]], axis=0)
        value = mm3((highs, lows), (d_high[sup], d_low[sup]))
        top = value[0:64]
        own_var[sup, :] = own_var[sup, :] + jnp.sum(top * top, axis=0)
        return value

    def put_mean(sup, rows):
        place = PLACE[sup][1]
        mean_out[sup] = rows[2 * place : 2 * place + 2]

    def products(everyone, group, slots, with_sums):
        gather_left(everyone, group)
        for side, slot in enumerate(slots):
            if slot is None:
                continue
            value = times_d(slot[0], side, with_sums)
            if with_sums:
                put_mean(slot[0], value[64:80])

    share2 = share_rows(all2, home2)
    next(share2)
    for _ in share1:
        pass
    products(all1, 0, FIRST[0], False)
    next(share2)
    products(all1, 1, FIRST[1], False)
    next(share2)
    products(all1, 2, FIRST[2], False)
    next(share2)
    next(share2, None)
    gather_sums(all2, 2)
    for group in range(2):
        products(all2, group, SECOND[group], True)
    for sup in (4, 5):
        side = PLACE[sup][0]
        put_mean(sup, mm3((x_high[side], x_low[side]), (d_high[sup], d_low[sup])))

    copies = []
    for step in range(1, 4):
        copies.append(copy_to(own_var, sums_x.at[step - 1], (y, k, z, (x + step) % 4)))
    for copy in copies:
        copy.wait_recv()
    sums_z[0] = own_var[...] + sums_x[0] + sums_x[1] + sums_x[2]
    copies = []
    for step in range(1, 8):
        copies.append(copy_to(sums_z.at[0], sums_z.at[step], (y, k, (z + step) % 8, x)))
    for copy in copies:
        copy.wait_recv()
    total = sums[...]
    for step in range(8):
        total = total + sums_z[step]
    var_out[...] = total[0:NS]
    while pending:
        pending.pop().wait_send()


def sweep(width, parent, marks, blocks, diag_inv, post):
    any_ = pl.BlockSpec(memory_space=pl.ANY)
    vmem = pl.BlockSpec(memory_space=pltpu.VMEM)
    smem = pl.BlockSpec(memory_space=pltpu.SMEM)
    return pl.pallas_call(
        functools.partial(sweep_kernel, width),
        out_shape=(jax.ShapeDtypeStruct((NS, 2, 256), F32), jax.ShapeDtypeStruct((NS, 256), F32)),
        in_specs=[smem, smem, any_, any_, vmem],
        out_specs=(vmem, vmem),
        scratch_shapes=[
            pltpu.VMEM((3, 4, 2, 256, 128), F32),
            pltpu.VMEM((2, 4, 2, 256, 128), F32),
            pltpu.VMEM((3, 4, 256, 128), F32),
            pltpu.VMEM((2, 4, 256, 128), F32),
            pltpu.VMEM((3, 2, 128, 128), F32),
            pltpu.VMEM((2, 2, 128, 128), F32),
            pltpu.VMEM((3, 2, 256, 128), F32),
            pltpu.VMEM((2, 2, 256, 128), F32),
            pltpu.VMEM((32, 3, 8, 128), F32),
            pltpu.VMEM((32, 3, 8, 128), F32),
            pltpu.VMEM((8, 32, 3, 8, 128), F32),
            pltpu.VMEM((8, 32, 3, 8, 128), F32),
            pltpu.VMEM((8, 32, 2, 8, 128), F32),
            pltpu.VMEM((8, 4, width * 128, 128), F32),
            pltpu.VMEM((3, 2048, 256), F32),
            pltpu.VMEM((NS, 2048, 256), BF16),
            pltpu.VMEM((NS, 2048, 256), BF16),
            pltpu.VMEM((NS, NS, 64, 256), F32),
            pltpu.VMEM((32, 16, 256), F32),
            pltpu.VMEM((NS, 256, 256), BF16),
            pltpu.VMEM((NS, 256, 256), BF16),
            pltpu.VMEM((2, 64, 2048), BF16),
            pltpu.VMEM((2, 64, 2048), BF16),
            pltpu.VMEM((2, 16, 2048), BF16),
            pltpu.VMEM((2, 16, 2048), BF16),
            pltpu.VMEM((width * 256, 2048), BF16),
            pltpu.VMEM((width * 256, 2048), BF16),
            pltpu.VMEM((16, 256), F32),
            pltpu.VMEM((8, 256), F32),
            pltpu.VMEM((8, 256), F32),
            pltpu.VMEM((3, 8, 256), F32),
            pltpu.VMEM((8, 8, 256), F32),
            pltpu.SemaphoreType.DMA((160,)),
            pltpu.SemaphoreType.DMA((160,)),
            pltpu.SemaphoreType.DMA((7,)),
        ],
        compiler_params=pltpu.CompilerParams(
            collective_id=width - 1, has_side_effects=True, vmem_limit_bytes=67_000_000
        ),
        cost_estimate=pl.CostEstimate(flops=12_000_000_000, bytes_accessed=30_000_000, transcendentals=0),
    )(parent, marks, blocks, diag_inv, post)


def body(factor, diag_inv, structure, parent, post):
    marks = jnp.transpose(structure, (0, 2, 1))
    blocks = jnp.transpose(factor, (0, 2, 3, 1))
    mean, variance = sweep(2, parent, marks, blocks, diag_inv, jnp.transpose(post, (0, 2, 1)))
    return jnp.transpose(mean, (0, 2, 1)), variance


def solution(mesh):
    finer = Mesh(mesh.devices.reshape(4, 2, 8, 4), ("y", "core", "z", "x"))
    row, col = ("y", "core"), ("z", "x")
    placed = (
        P(None, row, None, col),
        P(None, None, row),
        P(None, None, row),
        P(),
        P(None, row, col),
    )
    return jax.shard_map(
        body,
        mesh=finer,
        in_specs=placed,
        out_specs=(P(None, row, col), P(None, row)),
        check_vma=False,
    )
```

```python
import functools

import jax
import jax.numpy as jnp
from jax import lax
from jax.experimental import pallas as pl
from jax.experimental.pallas import tpu as pltpu
from jax.sharding import Mesh
from jax.sharding import PartitionSpec as P

NS = 6
MESH = pl.DeviceIdType.MESH
F32 = jnp.float32
BF16 = jnp.bfloat16
FIRST = (((4, 0), None), ((2, 0), (3, 0)), ((0, 0), (1, 0)))
SECOND = (((2, 1), (3, 1)), ((0, 1), (1, 1)))
PLACE = {4: (0, 0), 2: (0, 1), 0: (0, 2), 3: (1, 0), 1: (1, 1), 5: (1, 2)}
NT = (((1,), (1,)), ((), ()))
NN = (((1,), (0,)), ((), ()))


def halves(value):
    high = value.astype(BF16)
    return high, (value - high.astype(F32)).astype(BF16)


def mm(left, right, dims=NN):
    return lax.dot_general(left, right, dims, preferred_element_type=F32)


def mm3(left, right, dims=NN):
    return mm(left[0], right[0], dims) + mm(left[1], right[0], dims) + mm(left[0], right[1], dims)


def ancestor_of(parent, sup, second):
    first = parent[sup]
    if not second:
        return first
    return jnp.where(first < NS, parent[jnp.minimum(first, NS - 1)], NS)


def inner_flags(parent):
    flags = {}
    for sup in (4, 3, 2, 1):
        has_child = functools.reduce(jnp.logical_or, [parent[below] == sup for below in range(sup)])
        flags[sup] = jnp.logical_and(parent[sup] < NS, has_child).astype(jnp.int32)
    return flags


class Sems:
    def __init__(self, ref):
        self.ref, self.used = ref, 0

    def take(self):
        self.used += 1
        return self.ref.at[self.used - 1]


def sweep_kernel(
    early, parent, marks, blocks, diag_inv, post, mean_out, var_out,
    part1, part2, core1, core2, once1, once2, twice1, twice2, home1, home2, all1, all2, all_up,
    spread, d_raw, d_high, d_low, block_buf, post_all, post_high, post_low, l_high, l_low,
    x_high, x_low, h_high, h_low, post_rows, own_var, sums, sums_x, sums_z, sends, recvs, locals_,
):
    width = 1 if early else 2
    y, k = lax.axis_index("y"), lax.axis_index("core")
    z, x = lax.axis_index("z"), lax.axis_index("x")
    r, c = y * 2 + k, z * 4 + x
    up, down, over = (y + 1) % 4, (y + 3) % 4, (y + 2) % 4
    send_sems, recv_sems = Sems(sends), Sems(recvs)
    pending = []

    def copy_to(src, dst, device):
        copy = pltpu.make_async_remote_copy(
            src_ref=src, dst_ref=dst, send_sem=send_sems.take(), recv_sem=recv_sems.take(),
            device_id=device, device_id_type=MESH,
        )
        copy.start()
        pending.append(copy)
        return copy

    load_b = pltpu.make_async_copy(blocks, block_buf, locals_.at[6])
    load_b.start()
    d_order = (5, 4, 3, 2, 1, 0)

    def load_d(order):
        load = pltpu.make_async_copy(diag_inv.at[d_order[order]], d_raw.at[order % 3], locals_.at[order])
        load.start()
        return load

    d_loads = [load_d(order) for order in range(3)]

    barrier = pltpu.get_barrier_semaphore()

    def greet(step, carry):
        there = (c + step) % 32
        pl.semaphore_signal(barrier, inc=1, device_id=(y, k, there // 4, there % 4), device_id_type=MESH)
        return carry

    lax.fori_loop(1, 32, greet, 0)
    for device in ((up, k, z, x), (down, k, z, x), (y, 1 - k, z, x)):
        pl.semaphore_signal(barrier, inc=1, device_id=device, device_id_type=MESH)

    def to_columns(source, target):
        send_sem, recv_sem = send_sems.take(), recv_sems.take()

        def one(step, carry):
            there = (c + step) % 32
            pltpu.make_async_remote_copy(
                src_ref=source(there), dst_ref=target(c), send_sem=send_sem, recv_sem=recv_sem,
                device_id=(y, k, there // 4, there % 4), device_id_type=MESH,
            ).start()
            return carry

        lax.fori_loop(1, 32, one, 0)
        return send_sem, recv_sem

    def bulk(sources, target, sems):
        return pltpu.make_async_remote_copy(
            src_ref=sources, dst_ref=target, send_sem=sems[0], recv_sem=sems[1],
            device_id=(y, k, z, (x + 1) % 4), device_id_type=MESH,
        )

    def reduce_rows(part, core, once, twice, home, group):
        swaps = {}
        for name, there in (("over", over), ("up", up), ("down", down), ("own", y)):
            swaps[name] = copy_to(part.at[group, there, 1 - k], core.at[group, there], (y, 1 - k, z, x))
        yield
        swaps["over"].wait_recv()
        core[group, over] += part[group, over, k]
        one_up = copy_to(core.at[group, over, pl.ds(0, 128)], once.at[group, 0], (up, k, z, x))
        one_down = copy_to(core.at[group, over, pl.ds(128, 128)], once.at[group, 1], (down, k, z, x))
        for name, there in (("up", up), ("down", down), ("own", y)):
            swaps[name].wait_recv()
            core[group, there] += part[group, there, k]
        yield
        one_up.wait_recv()
        core[group, up, 0:128] += once[group, 0]
        two_up = copy_to(core.at[group, up], twice.at[group, 0], (up, k, z, x))
        one_down.wait_recv()
        core[group, down, 128:256] += once[group, 1]
        two_down = copy_to(core.at[group, down], twice.at[group, 1], (down, k, z, x))
        yield
        two_up.wait_recv()
        two_down.wait_recv()
        value = core[group, y] + twice[group, 0] + twice[group, 1]
        home[group] = value.reshape(32, 8, 128)

    def over_rows(everyone):
        below, above, beyond = down * 2 + k, up * 2 + k, over * 2 + k
        to_up = copy_to(everyone.at[r], everyone.at[r], (up, k, z, x))
        to_down = copy_to(everyone.at[r], everyone.at[r], (down, k, z, x))
        across = [copy_to(everyone.at[r], everyone.at[r], (y, 1 - k, z, x))]
        yield
        lower, upper = pl.ds(0, 16), pl.ds(16, 16)
        to_up.wait_recv()
        on_up = copy_to(everyone.at[below, lower], everyone.at[below, lower], (up, k, z, x))
        across.append(copy_to(everyone.at[below], everyone.at[below], (y, 1 - k, z, x)))
        to_down.wait_recv()
        on_down = copy_to(everyone.at[above, upper], everyone.at[above, upper], (down, k, z, x))
        across.append(copy_to(everyone.at[above], everyone.at[above], (y, 1 - k, z, x)))
        yield
        on_up.wait_recv()
        on_down.wait_recv()
        across.append(copy_to(everyone.at[beyond], everyone.at[beyond], (y, 1 - k, z, x)))
        yield
        for copy in across:
            copy.wait_recv()

    def exchange(everyone, home, tile):
        everyone[tile, r, c] = home[tile, c]
        return to_columns(lambda there: home.at[tile, there], lambda here: everyone.at[tile, r, here])

    def share(everyone, home, tile, sems):
        both = bulk(home.at[tile, pl.ds(0, 31)], everyone.at[tile, r, pl.ds(0, 31)], sems)
        both.wait_recv()
        pending.append(both)
        yield from over_rows(everyone.at[tile])

    def ring(size, me, device, chunk):
        ahead, behind = (me + 1) % size, (me + size - 1) % size
        forth = [copy_to(chunk(me, q), chunk(me, q), device(ahead)) for q in range(2)]
        back = [copy_to(chunk(me, q), chunk(me, q), device(behind)) for q in (1, 0)][::-1]
        yield
        for step in range(1, size // 2):
            last = step == size // 2 - 1
            got_low, got_high = (me + size - step) % size, (me + step) % size
            for q in range(2):
                forth[q].wait_recv()
                if not last or q == 0:
                    low = chunk(got_low, q)
                    forth[q] = copy_to(low, low, device(ahead))
                back[1 - q].wait_recv()
                if not last or q == 0:
                    high = chunk(got_high, 1 - q)
                    back[1 - q] = copy_to(high, high, device(behind))
            yield
        forth[0].wait_recv()
        back[1].wait_recv()

    def chained(*generators):
        for generator in generators:
            yield from generator()

    def run_together(generators, beside=()):
        live = list(generators)
        while live:
            for generator in list(live):
                if next(generator, "end") == "end":
                    live.remove(generator)
            for generator in beside:
                next(generator, None)

    row_of = lax.broadcasted_iota(jnp.int32, (64, 256), 0)
    col_of = lax.broadcasted_iota(jnp.int32, (64, 256), 1) + r * 256

    def split_d(order):
        sup = d_order[order]
        d_loads[order].wait()

        def one(piece, total):
            rows = pl.ds(pl.multiple_of(piece * 64, 64), 64)
            value = jnp.where(row_of + piece * 64 >= col_of, d_raw[order % 3, rows, :], 0.0)
            high, low = halves(value)
            d_high[sup, rows, :] = high
            d_low[sup, rows, :] = low
            return total + jnp.sum((value * value).reshape(8, 8, 256), axis=0)

        total = lax.fori_loop(0, 32, one, jnp.zeros((8, 256), F32), unroll=2)
        sums[sup, :] = jnp.sum(total, axis=0)
        if order + 3 < NS:
            d_loads.append(load_d(order + 3))

    split_d(0)
    load_b.wait()

    row_lane = lax.broadcasted_iota(jnp.int32, (64, 256), 1)

    def multiply(part, group, slots):
        nothing = jnp.zeros((64, 256), F32)
        lane = lax.broadcasted_iota(jnp.int32, (256, 256), 1)
        targets, weights = [], []
        for side, slot in enumerate(slots):
            if slot is None:
                continue
            sup, second = slot
            target = ancestor_of(parent, sup, second)
            valid = target < NS
            at = jnp.minimum(target, NS - 1)
            upper_mark = jnp.where(valid, marks[sup, 0, at], 0).astype(F32)
            lower_mark = jnp.where(valid, marks[sup, 1, at], 0).astype(F32)
            block = block_buf[at, sup] * jnp.where(row_lane < 128, upper_mark, lower_mark)
            high = block.astype(BF16).astype(F32)
            low = block - high
            rows = [high, nothing, low, nothing] if side == 0 else [nothing, high, nothing, low]
            both = jnp.concatenate(rows, axis=0).T
            targets.append(at)
            weights += [both.astype(BF16), jnp.where(lane < 128, both, 0.0).astype(BF16)]
        right = jnp.concatenate(weights, axis=0)

        def one(piece, carry):
            rows = pl.ds(pl.multiple_of(piece * 512, 512), 512)
            left = [d_ref[at, rows, :] for at in targets for d_ref in (d_high, d_low)]
            total = mm(jnp.concatenate(left, axis=1), right)
            value = total[:, :128] + total[:, 128:]
            part[group, piece, 0] = value[0:256]
            part[group, piece, 1] = value[256:512]
            return carry

        lax.fori_loop(0, 4, one, 0)

    sums1 = [reduce_rows(part1, core1, once1, twice1, home1, group) for group in range(3)]
    sums2 = [reduce_rows(part2, core2, once2, twice2, home2, group) for group in range(2)]
    own_var[...] = jnp.zeros_like(own_var)
    multiply(part1, 0, FIRST[0])
    for sup in range(NS):
        post_rows[2 * sup : 2 * sup + 2, :] = post[sup]
    post_rows[2 * NS : 16, :] = jnp.zeros((16 - 2 * NS, 256), F32)
    pl.semaphore_wait(barrier, 34)
    next(sums1[0])
    post_all[c] = post_rows[...]
    post_sems = to_columns(lambda there: post_rows, lambda here: post_all.at[here])
    if early:
        split_d(1)
        next(sums1[0])
        split_d(2)
        multiply(part1, 1, FIRST[1])
        next(sums1[1])
        next(sums1[0])
        split_d(3)
        next(sums1[0], None)
        moved1 = [None] * 3
    else:
        split_d(1)
        next(sums1[0])
        split_d(2)
        multiply(part1, 1, FIRST[1])
        next(sums1[1])
        next(sums1[0])
        split_d(3)
        next(sums1[1])
        split_d(4)
        multiply(part1, 2, FIRST[2])
        next(sums1[2])
        next(sums1[0], None)
        moved1 = [exchange(all1, home1, 0)]
        next(sums1[1])
        next(sums1[2])
        multiply(part2, 0, SECOND[0])
        next(sums2[0])
        next(sums1[1], None)
        moved1.append(exchange(all1, home1, 1))
        next(sums1[2])
        multiply(part2, 1, SECOND[1])
        next(sums2[1])
        next(sums1[2], None)

    flags = inner_flags(parent)
    picks = []
    before = jnp.int32(0)
    for sup in (4, 3, 2, 1):
        picks.append((sup, [flags[sup] * (before == place).astype(jnp.int32) for place in range(width)]))
        before = before + flags[sup]
    where_of = {4: (0, 0), 2: (1, 0), 3: (1, 1), 1: (2, 1)}
    low_lanes = lax.broadcasted_iota(jnp.int32, (256, 128), 1) < 64
    rolled = lambda value: pltpu.roll(value, 64, 1)
    if early:
        value = home1[0].reshape(256, 128)
        spread[z, x] = jnp.where(low_lanes[0:128], value[0:128], rolled(value[128:256]))
    else:
        firsts = [home1[tile].reshape(256, 128) for tile in range(3)]
        chosen = []
        for place in range(2):
            sides = [jnp.zeros((256, 128), F32), jnp.zeros((256, 128), F32)]
            for sup, weight in picks:
                tile, side = where_of[sup]
                sides[side] = sides[side] + firsts[tile] * weight[place].astype(F32)
            chosen.append(sides)
        lo = chosen[0][0] + rolled(chosen[0][1])
        hi = rolled(chosen[1][0]) + chosen[1][1]
        spread[z, x] = jnp.where(low_lanes, lo, hi)

    size = width * 128
    quarter = size // 4
    on_z = lambda there: (y, k, there, x)
    on_x = lambda there: (y, k, z, there)
    quarter_of = lambda part_at: pl.ds(part_at * quarter, quarter)
    order_a = chained(
        lambda: ring(8, z, on_z, lambda i, q: spread.at[i, x, quarter_of(q)]),
        lambda: ring(4, x, on_x, lambda i, q: spread.at[:, i, quarter_of(q)]),
    )
    order_b = chained(
        lambda: ring(4, x, on_x, lambda i, q: spread.at[z, i, quarter_of(2 + q)]),
        lambda: ring(8, z, on_z, lambda i, q: spread.at[i, :, quarter_of(2 + q)]),
    )

    def up_copies(tile):
        all_up[tile, r] = home1[1 + tile]
        yield from over_rows(all_up.at[tile])

    pair_of = (lax.broadcasted_iota(jnp.int32, (256, 128), 0) % 8) // 2

    def placed(sup, value):
        side, pair = PLACE[sup]
        here = low_lanes if side == 0 else jnp.logical_not(low_lanes)
        return jnp.where(here & (pair_of == pair), value, 0.0)

    right_sum = [jnp.zeros((256, 128), F32)]

    def minus_post(home, group, slots):
        parts = halves(home[group].reshape(256, 128))
        for slot in slots:
            if slot is None:
                continue
            sup, second = slot
            at = jnp.minimum(ancestor_of(parent, sup, second), NS - 1)
            value = mm3((post_high[at], post_low[at]), parts)
            right_sum[0] = right_sum[0] - placed(sup, value)

    def right_sides(rounds):
        for _ in range(rounds):
            yield
        split_d(5)
        yield
        post_both = bulk(post_all.at[pl.ds(0, 31)], post_all.at[pl.ds(0, 31)], post_sems)
        post_both.wait_recv()
        pending.append(post_both)
        for sup in range(NS):
            rows = post_all[:, 2 * sup : 2 * sup + 2, :]
            value = jnp.concatenate([rows] * 4, axis=1).reshape(256, 256)
            high, low = halves(value)
            post_high[sup] = high
            post_low[sup] = low
        yield
        pick_row = lax.broadcasted_iota(jnp.int32, (256, 128), 0)
        pick_col = lax.broadcasted_iota(jnp.int32, (256, 128), 1) % 64 + x * 64
        picker = jnp.where((pick_row == pick_col) & (r == c // 4), 1.0, 0.0).astype(BF16)
        for sup in range(NS):
            value = mm(post_high[sup], picker) + mm(post_low[sup], picker)
            right_sum[0] = right_sum[0] + placed(sup, value)
        yield
        for group in range(3):
            minus_post(home1, group, FIRST[group])

    def last_exchange():
        yield
        yield
        moved1.append(exchange(all1, home1, 2))

    def first_copies(rounds):
        for _ in range(rounds):
            yield
        yield from share(all1, home1, 0, moved1[0])
        yield from share(all1, home1, 1, moved1[1])

    def last_copies():
        yield from share(all1, home1, 2, moved1[2])

    def chain_one():
        yield from sums1[1]
        moved1[1] = exchange(all1, home1, 1)
        yield from up_copies(0)

    def chain_two():
        split_d(4)
        multiply(part1, 2, FIRST[2])
        yield from sums1[2]
        moved1[2] = exchange(all1, home1, 2)
        yield from up_copies(1)

    def chain_three():
        yield
        moved1[0] = exchange(all1, home1, 0)
        multiply(part2, 0, SECOND[0])
        yield from sums2[0]

    def chain_four():
        yield
        yield
        multiply(part2, 1, SECOND[1])
        yield from sums2[1]

    if early:
        beside = [first_copies(7)]
        run_together(
            (order_a, order_b, chain_one(), chain_two(), chain_three(), chain_four(), right_sides(4)),
            beside,
        )
    else:
        beside = [first_copies(3)]
        run_together(
            (order_a, order_b, sums2[0], sums2[1], up_copies(0), up_copies(1), last_exchange(), right_sides(0)),
            beside,
        )

    def merge(pair, carry):
        cols = pl.ds(pl.multiple_of(pair * 128, 128), 128)
        even = spread[pair // 2, 2 * (pair % 2)]
        odd = spread[pair // 2, 2 * (pair % 2) + 1]
        wide = low_lanes[0:size]
        for side, value in (
            (0, jnp.where(wide, even, rolled(odd))),
            (1, jnp.where(wide, rolled(even), odd)),
        ):
            high, low = halves(value)
            rows = pl.ds(side * size, size)
            h_high[rows, cols] = high
            h_low[rows, cols] = low
        return carry

    lax.fori_loop(0, 16, merge, 0)
    lane_256 = lax.broadcasted_iota(jnp.int32, (1, 256), 1)
    through = jnp.zeros((256, 256), F32)
    for place in range(width):
        keep = jnp.zeros((1, 256), F32)
        for at, sup in enumerate((2, 3, 0, 1)):
            chosen_here = jnp.int32(0)
            for inner_sup, weight in picks:
                if inner_sup > sup:
                    chosen_here = chosen_here + weight[place] * (parent[sup] == inner_sup).astype(jnp.int32)
            keep = keep + jnp.where(lane_256 // 64 == at, chosen_here.astype(F32), 0.0)
        for row_block in range(8):
            right = jnp.concatenate(
                [all_up[tile, row_block].reshape(256, 128) for tile in range(2)], axis=1
            )
            cols = pl.ds(row_block * 256, 256)
            rows = pl.ds(place * 256, 256)
            through = through + mm3((h_high[rows, cols], h_low[rows, cols]), halves(right * keep))
    moved2 = []
    for group in range(2):
        value = home2[group].reshape(256, 128) - through[:, group * 128 : group * 128 + 128]
        home2[group] = value.reshape(32, 8, 128)
        moved2.append(exchange(all2, home2, group))
    for group in range(2):
        minus_post(home2, group, SECOND[group])
    home2[2] = right_sum[0].reshape(32, 8, 128)
    moved2.append(exchange(all2, home2, 2))

    lane64 = low_lanes[0:64]
    lane8 = low_lanes[0:8]

    def gather_left(everyone, group):
        def one(pair, carry):
            even = everyone[group, :, 2 * pair].reshape(64, 128)
            odd = everyone[group, :, 2 * pair + 1].reshape(64, 128)
            cols = pl.ds(pl.multiple_of(pair * 128, 128), 128)
            for side, value in (
                (0, jnp.where(lane64, even, rolled(odd))),
                (1, jnp.where(lane64, rolled(even), odd)),
            ):
                high, low = halves(value)
                l_high[side, 0:64, cols] = high
                l_low[side, 0:64, cols] = low
            return carry

        lax.fori_loop(0, 16, one, 0, unroll=2)

    def gather_sums(everyone, group):
        for pair in range(16):
            even = jnp.sum(everyone[group, :, 2 * pair], axis=0)
            odd = jnp.sum(everyone[group, :, 2 * pair + 1], axis=0)
            cols = pl.ds(pair * 128, 128)
            blank = jnp.zeros((8, 128), F32)
            for side, value in (
                (0, jnp.where(lane8, even, rolled(odd))),
                (1, jnp.where(lane8, rolled(even), odd)),
            ):
                high, low = halves(jnp.concatenate([value, blank], axis=0))
                x_high[side, :, cols] = high
                x_low[side, :, cols] = low

    def times_d(sup, side, with_sums):
        highs, lows = l_high[side], l_low[side]
        if with_sums:
            highs = jnp.concatenate([highs, x_high[side]], axis=0)
            lows = jnp.concatenate([lows, x_low[side]], axis=0)
        value = mm3((highs, lows), (d_high[sup], d_low[sup]))
        top = value[0:64]
        own_var[sup, :] = own_var[sup, :] + jnp.sum(top * top, axis=0)
        return value

    def put_mean(sup, rows):
        place = PLACE[sup][1]
        mean_out[sup] = rows[2 * place : 2 * place + 2]

    def products(everyone, group, slots, with_sums):
        gather_left(everyone, group)
        for side, slot in enumerate(slots):
            if slot is None:
                continue
            value = times_d(slot[0], side, with_sums)
            if with_sums:
                put_mean(slot[0], value[64:80])

    share2 = [share(all2, home2, tile, moved2[tile]) for tile in range(3)]
    run_together(beside + [last_copies()] + share2)
    for tile in range(3):
        products(all1, tile, FIRST[tile], False)
    gather_sums(all2, 2)
    for group in range(2):
        products(all2, group, SECOND[group], True)
    for sup in (4, 5):
        side = PLACE[sup][0]
        put_mean(sup, mm3((x_high[side], x_low[side]), (d_high[sup], d_low[sup])))

    copies = []
    for step in range(1, 4):
        copies.append(copy_to(own_var, sums_x.at[step - 1], (y, k, z, (x + step) % 4)))
    for copy in copies:
        copy.wait_recv()
    sums_z[0] = own_var[...] + sums_x[0] + sums_x[1] + sums_x[2]
    copies = []
    for step in range(1, 8):
        copies.append(copy_to(sums_z.at[0], sums_z.at[step], (y, k, (z + step) % 8, x)))
    for copy in copies:
        copy.wait_recv()
    total = sums[...]
    for step in range(8):
        total = total + sums_z[step]
    var_out[...] = total[0:NS]
    while pending:
        pending.pop().wait_send()


def sweep(early, parent, marks, blocks, diag_inv, post):
    width = 1 if early else 2
    any_ = pl.BlockSpec(memory_space=pl.ANY)
    vmem = pl.BlockSpec(memory_space=pltpu.VMEM)
    smem = pl.BlockSpec(memory_space=pltpu.SMEM)
    return pl.pallas_call(
        functools.partial(sweep_kernel, early),
        out_shape=(jax.ShapeDtypeStruct((NS, 2, 256), F32), jax.ShapeDtypeStruct((NS, 256), F32)),
        in_specs=[smem, smem, any_, any_, vmem],
        out_specs=(vmem, vmem),
        scratch_shapes=[
            pltpu.VMEM((3, 4, 2, 256, 128), F32),
            pltpu.VMEM((2, 4, 2, 256, 128), F32),
            pltpu.VMEM((3, 4, 256, 128), F32),
            pltpu.VMEM((2, 4, 256, 128), F32),
            pltpu.VMEM((3, 2, 128, 128), F32),
            pltpu.VMEM((2, 2, 128, 128), F32),
            pltpu.VMEM((3, 2, 256, 128), F32),
            pltpu.VMEM((2, 2, 256, 128), F32),
            pltpu.VMEM((3, 32, 8, 128), F32),
            pltpu.VMEM((3, 32, 8, 128), F32),
            pltpu.VMEM((3, 8, 32, 8, 128), F32),
            pltpu.VMEM((3, 8, 32, 8, 128), F32),
            pltpu.VMEM((2, 8, 32, 8, 128), F32),
            pltpu.VMEM((8, 4, width * 128, 128), F32),
            pltpu.VMEM((3, 2048, 256), F32),
            pltpu.VMEM((NS, 2048, 256), BF16),
            pltpu.VMEM((NS, 2048, 256), BF16),
            pltpu.VMEM((NS, NS, 64, 256), F32),
            pltpu.VMEM((32, 16, 256), F32),
            pltpu.VMEM((NS, 256, 256), BF16),
            pltpu.VMEM((NS, 256, 256), BF16),
            pltpu.VMEM((2, 64, 2048), BF16),
            pltpu.VMEM((2, 64, 2048), BF16),
            pltpu.VMEM((2, 16, 2048), BF16),
            pltpu.VMEM((2, 16, 2048), BF16),
            pltpu.VMEM((width * 256, 2048), BF16),
            pltpu.VMEM((width * 256, 2048), BF16),
            pltpu.VMEM((16, 256), F32),
            pltpu.VMEM((8, 256), F32),
            pltpu.VMEM((8, 256), F32),
            pltpu.VMEM((3, 8, 256), F32),
            pltpu.VMEM((8, 8, 256), F32),
            pltpu.SemaphoreType.DMA((200,)),
            pltpu.SemaphoreType.DMA((200,)),
            pltpu.SemaphoreType.DMA((7,)),
        ],
        compiler_params=pltpu.CompilerParams(
            collective_id=int(early), has_side_effects=True, vmem_limit_bytes=67_000_000
        ),
        cost_estimate=pl.CostEstimate(flops=12_000_000_000, bytes_accessed=30_000_000, transcendentals=0),
    )(parent, marks, blocks, diag_inv, post)


def body(factor, diag_inv, structure, parent, post):
    marks = jnp.transpose(structure, (0, 2, 1))
    blocks = jnp.transpose(factor, (0, 2, 3, 1))
    flags = inner_flags(parent)
    only_four = (flags[4] == 1) & (flags[3] + flags[2] + flags[1] == 0)
    mean, variance = lax.cond(
        only_four,
        functools.partial(sweep, True),
        functools.partial(sweep, False),
        parent, marks, blocks, diag_inv, jnp.transpose(post, (0, 2, 1)),
    )
    return jnp.transpose(mean, (0, 2, 1)), variance


def solution(mesh):
    finer = Mesh(mesh.devices.reshape(4, 2, 8, 4), ("y", "core", "z", "x"))
    row, col = ("y", "core"), ("z", "x")
    placed = (
        P(None, row, None, col),
        P(None, None, row),
        P(None, None, row),
        P(),
        P(None, row, col),
    )
    return jax.shard_map(
        body,
        mesh=finer,
        in_specs=placed,
        out_specs=(P(None, row, col), P(None, row)),
        check_vma=False,
    )
```

```python
import functools

import jax
import jax.numpy as jnp
from jax import lax
from jax.experimental import pallas as pl
from jax.experimental.pallas import tpu as pltpu
from jax.sharding import Mesh
from jax.sharding import PartitionSpec as P

NS = 6
MESH = pl.DeviceIdType.MESH
F32 = jnp.float32
BF16 = jnp.bfloat16
FIRST = (((4, 0), None), ((2, 0), (3, 0)), ((0, 0), (1, 0)))
SECOND = (((2, 1), (3, 1)), ((0, 1), (1, 1)))
PLACE = {4: (0, 0), 2: (0, 1), 0: (0, 2), 3: (1, 0), 1: (1, 1), 5: (1, 2)}
NT = (((1,), (1,)), ((), ()))
NN = (((1,), (0,)), ((), ()))


def halves(value):
    high = value.astype(BF16)
    return high, (value - high.astype(F32)).astype(BF16)


def mm(left, right, dims=NN):
    return lax.dot_general(left, right, dims, preferred_element_type=F32)


def mm3(left, right, dims=NN):
    size = left[0].shape[0]
    both = mm(jnp.concatenate(left, axis=0), right[0], dims)
    return both[:size] + both[size:] + mm(left[0], right[1], dims)


def ancestor_of(parent, sup, second):
    first = parent[sup]
    if not second:
        return first
    return jnp.where(first < NS, parent[jnp.minimum(first, NS - 1)], NS)


def inner_flags(parent):
    flags = {}
    for sup in (4, 3, 2, 1):
        has_child = functools.reduce(jnp.logical_or, [parent[below] == sup for below in range(sup)])
        flags[sup] = jnp.logical_and(parent[sup] < NS, has_child).astype(jnp.int32)
    return flags


class Sems:
    def __init__(self, ref):
        self.ref, self.used = ref, 0

    def take(self):
        self.used += 1
        return self.ref.at[self.used - 1]


def sweep_kernel(
    width, parent, marks, blocks, diag_inv, post, mean_out, var_out,
    part1, part2, core1, core2, once1, once2, twice1, twice2, home1, home2, all1, all2, all_up,
    spread, d_raw, d_high, d_low, block_buf, post_all, post_high, post_low, l_high, l_low,
    x_high, x_low, h_high, h_low, post_rows, own_var, sums, sums_x, sums_z, sends, recvs, locals_,
):
    y, k = lax.axis_index("y"), lax.axis_index("core")
    z, x = lax.axis_index("z"), lax.axis_index("x")
    r, c = y * 2 + k, z * 4 + x
    up, down, over = (y + 1) % 4, (y + 3) % 4, (y + 2) % 4
    send_sems, recv_sems = Sems(sends), Sems(recvs)
    pending = []

    def copy_to(src, dst, device):
        copy = pltpu.make_async_remote_copy(
            src_ref=src, dst_ref=dst, send_sem=send_sems.take(), recv_sem=recv_sems.take(),
            device_id=device, device_id_type=MESH,
        )
        copy.start()
        pending.append(copy)
        return copy

    load_b = pltpu.make_async_copy(blocks, block_buf, locals_.at[6])
    load_b.start()
    d_order = (5, 4, 3, 2, 1, 0)

    def load_d(order):
        load = pltpu.make_async_copy(diag_inv.at[d_order[order]], d_raw.at[order % 3], locals_.at[order])
        load.start()
        return load

    d_loads = [load_d(order) for order in range(3)]

    barrier = pltpu.get_barrier_semaphore()

    def greet(step, carry):
        there = (c + step) % 32
        pl.semaphore_signal(barrier, inc=1, device_id=(y, k, there // 4, there % 4), device_id_type=MESH)
        return carry

    lax.fori_loop(1, 32, greet, 0)
    for device in ((up, k, z, x), (down, k, z, x), (y, 1 - k, z, x)):
        pl.semaphore_signal(barrier, inc=1, device_id=device, device_id_type=MESH)

    def to_columns(source, target):
        send_sem, recv_sem = send_sems.take(), recv_sems.take()

        def one(step, carry):
            there = (c + step) % 32
            pltpu.make_async_remote_copy(
                src_ref=source(there), dst_ref=target(c), send_sem=send_sem, recv_sem=recv_sem,
                device_id=(y, k, there // 4, there % 4), device_id_type=MESH,
            ).start()
            return carry

        lax.fori_loop(1, 32, one, 0)
        return send_sem, recv_sem

    def bulk(sources, target, sems):
        return pltpu.make_async_remote_copy(
            src_ref=sources, dst_ref=target, send_sem=sems[0], recv_sem=sems[1],
            device_id=(y, k, z, (x + 1) % 4), device_id_type=MESH,
        )

    def reduce_rows(part, core, once, twice, home, group):
        swaps = {}
        for name, there in (("over", over), ("up", up), ("down", down), ("own", y)):
            swaps[name] = copy_to(part.at[group, there, 1 - k], core.at[group, there], (y, 1 - k, z, x))
        yield
        swaps["over"].wait_recv()
        core[group, over] += part[group, over, k]
        one_up = copy_to(core.at[group, over, pl.ds(0, 128)], once.at[group, 0], (up, k, z, x))
        one_down = copy_to(core.at[group, over, pl.ds(128, 128)], once.at[group, 1], (down, k, z, x))
        for name, there in (("up", up), ("down", down), ("own", y)):
            swaps[name].wait_recv()
            core[group, there] += part[group, there, k]
        yield
        one_up.wait_recv()
        core[group, up, 0:128] += once[group, 0]
        two_up = copy_to(core.at[group, up], twice.at[group, 0], (up, k, z, x))
        one_down.wait_recv()
        core[group, down, 128:256] += once[group, 1]
        two_down = copy_to(core.at[group, down], twice.at[group, 1], (down, k, z, x))
        yield
        two_up.wait_recv()
        two_down.wait_recv()
        value = core[group, y] + twice[group, 0] + twice[group, 1]
        home[group] = value.reshape(32, 8, 128)

    def over_rows(everyone):
        below, above, beyond = down * 2 + k, up * 2 + k, over * 2 + k
        to_up = copy_to(everyone.at[r], everyone.at[r], (up, k, z, x))
        to_down = copy_to(everyone.at[r], everyone.at[r], (down, k, z, x))
        across = [copy_to(everyone.at[r], everyone.at[r], (y, 1 - k, z, x))]
        yield
        lower, upper = pl.ds(0, 16), pl.ds(16, 16)
        to_up.wait_recv()
        on_up = copy_to(everyone.at[below, lower], everyone.at[below, lower], (up, k, z, x))
        across.append(copy_to(everyone.at[below], everyone.at[below], (y, 1 - k, z, x)))
        to_down.wait_recv()
        on_down = copy_to(everyone.at[above, upper], everyone.at[above, upper], (down, k, z, x))
        across.append(copy_to(everyone.at[above], everyone.at[above], (y, 1 - k, z, x)))
        yield
        on_up.wait_recv()
        on_down.wait_recv()
        across.append(copy_to(everyone.at[beyond], everyone.at[beyond], (y, 1 - k, z, x)))
        yield
        for copy in across:
            copy.wait_recv()

    def exchange(everyone, home, tile):
        everyone[tile, r, c] = home[tile, c]
        return to_columns(lambda there: home.at[tile, there], lambda here: everyone.at[tile, r, here])

    def share(everyone, home, tile, sems):
        both = bulk(home.at[tile, pl.ds(0, 31)], everyone.at[tile, r, pl.ds(0, 31)], sems)
        both.wait_recv()
        pending.append(both)
        yield from over_rows(everyone.at[tile])

    def ring(size, me, device, chunk):
        ahead, behind = (me + 1) % size, (me + size - 1) % size
        forth = [copy_to(chunk(me, q), chunk(me, q), device(ahead)) for q in range(2)]
        back = [copy_to(chunk(me, q), chunk(me, q), device(behind)) for q in (1, 0)][::-1]
        yield
        for step in range(1, size // 2):
            last = step == size // 2 - 1
            got_low, got_high = (me + size - step) % size, (me + step) % size
            for q in range(2):
                forth[q].wait_recv()
                if not last or q == 0:
                    low = chunk(got_low, q)
                    forth[q] = copy_to(low, low, device(ahead))
                back[1 - q].wait_recv()
                if not last or q == 0:
                    high = chunk(got_high, 1 - q)
                    back[1 - q] = copy_to(high, high, device(behind))
            yield
        forth[0].wait_recv()
        back[1].wait_recv()

    def chained(*generators):
        for generator in generators:
            yield from generator()

    def run_together(generators, beside=()):
        live = list(generators)
        while live:
            for generator in list(live):
                if next(generator, "end") == "end":
                    live.remove(generator)
            for generator in beside:
                next(generator, None)

    row_of = lax.broadcasted_iota(jnp.int32, (64, 256), 0)
    col_of = lax.broadcasted_iota(jnp.int32, (64, 256), 1) + r * 256

    def split_d(order):
        sup = d_order[order]
        d_loads[order].wait()

        def one(piece, total):
            rows = pl.ds(pl.multiple_of(piece * 64, 64), 64)
            value = jnp.where(row_of + piece * 64 >= col_of, d_raw[order % 3, rows, :], 0.0)
            high, low = halves(value)
            d_high[sup, rows, :] = high
            d_low[sup, rows, :] = low
            return total + jnp.sum((value * value).reshape(8, 8, 256), axis=0)

        total = lax.fori_loop(0, 32, one, jnp.zeros((8, 256), F32), unroll=2)
        sums[sup, :] = jnp.sum(total, axis=0)
        if order + 3 < NS:
            d_loads.append(load_d(order + 3))

    split_d(0)
    load_b.wait()

    row_lane = lax.broadcasted_iota(jnp.int32, (64, 256), 1)

    def multiply(part, group, slots):
        nothing = jnp.zeros((64, 256), F32)
        lane = lax.broadcasted_iota(jnp.int32, (256, 256), 1)
        targets, weights = [], []
        for side, slot in enumerate(slots):
            if slot is None:
                continue
            sup, second = slot
            target = ancestor_of(parent, sup, second)
            valid = target < NS
            at = jnp.minimum(target, NS - 1)
            upper_mark = jnp.where(valid, marks[sup, 0, at], 0).astype(F32)
            lower_mark = jnp.where(valid, marks[sup, 1, at], 0).astype(F32)
            block = block_buf[at, sup] * jnp.where(row_lane < 128, upper_mark, lower_mark)
            high = block.astype(BF16).astype(F32)
            low = block - high
            rows = [high, nothing, low, nothing] if side == 0 else [nothing, high, nothing, low]
            both = jnp.concatenate(rows, axis=0).T
            targets.append(at)
            weights += [both.astype(BF16), jnp.where(lane < 128, both, 0.0).astype(BF16)]
        right = jnp.concatenate(weights, axis=0)
        for piece in range(4):
            rows = pl.ds(piece * 512, 512)
            left = [d_ref[at, rows, :] for at in targets for d_ref in (d_high, d_low)]
            total = mm(jnp.concatenate(left, axis=1), right)
            value = total[:, :128] + total[:, 128:]
            part[group, piece, 0] = value[0:256]
            part[group, piece, 1] = value[256:512]

    sums1 = [reduce_rows(part1, core1, once1, twice1, home1, group) for group in range(3)]
    sums2 = [reduce_rows(part2, core2, once2, twice2, home2, group) for group in range(2)]
    own_var[...] = jnp.zeros_like(own_var)
    multiply(part1, 0, FIRST[0])
    for sup in range(NS):
        post_rows[2 * sup : 2 * sup + 2, :] = post[sup]
    post_rows[2 * NS : 16, :] = jnp.zeros((16 - 2 * NS, 256), F32)
    pl.semaphore_wait(barrier, 34)
    next(sums1[0])
    post_all[c] = post_rows[...]
    post_sems = to_columns(lambda there: post_rows, lambda here: post_all.at[here])
    split_d(1)
    next(sums1[0])
    split_d(2)
    multiply(part1, 1, FIRST[1])
    next(sums1[1])
    next(sums1[0])
    split_d(3)
    next(sums1[1])
    split_d(4)
    multiply(part1, 2, FIRST[2])
    next(sums1[2])
    next(sums1[0], None)
    moved1 = [exchange(all1, home1, 0)]
    next(sums1[1])
    next(sums1[2])
    multiply(part2, 0, SECOND[0])
    next(sums2[0])
    next(sums1[1], None)
    moved1.append(exchange(all1, home1, 1))
    next(sums1[2])
    multiply(part2, 1, SECOND[1])
    next(sums2[1])
    next(sums1[2], None)

    flags = inner_flags(parent)
    picks = []
    before = jnp.int32(0)
    for sup in (4, 3, 2, 1):
        picks.append((sup, [flags[sup] * (before == place).astype(jnp.int32) for place in range(width)]))
        before = before + flags[sup]
    where_of = {4: (0, 0), 2: (1, 0), 3: (1, 1), 1: (2, 1)}
    low_lanes = lax.broadcasted_iota(jnp.int32, (256, 128), 1) < 64
    firsts = [home1[tile].reshape(256, 128) for tile in range(3)]
    chosen = []
    for place in range(width):
        sides = [jnp.zeros((256, 128), F32), jnp.zeros((256, 128), F32)]
        for sup, weight in picks:
            tile, side = where_of[sup]
            sides[side] = sides[side] + firsts[tile] * weight[place].astype(F32)
        chosen.append(sides)
    rolled = lambda value: pltpu.roll(value, 64, 1)
    if width == 1:
        lo, hi = chosen[0]
        in_low = jnp.where(low_lanes, lo + rolled(hi), 0.0)
        spread[z, x] = jnp.where(low_lanes[0:128], in_low[0:128], rolled(in_low[128:256]))
    else:
        lo = chosen[0][0] + rolled(chosen[0][1])
        hi = rolled(chosen[1][0]) + chosen[1][1]
        spread[z, x] = jnp.where(low_lanes, lo, hi)

    size = width * 128
    quarter = size // 4
    on_z = lambda there: (y, k, there, x)
    on_x = lambda there: (y, k, z, there)
    quarter_of = lambda part_at: pl.ds(part_at * quarter, quarter)
    order_a = chained(
        lambda: ring(8, z, on_z, lambda i, q: spread.at[i, x, quarter_of(q)]),
        lambda: ring(4, x, on_x, lambda i, q: spread.at[:, i, quarter_of(q)]),
    )
    order_b = chained(
        lambda: ring(4, x, on_x, lambda i, q: spread.at[z, i, quarter_of(2 + q)]),
        lambda: ring(8, z, on_z, lambda i, q: spread.at[i, :, quarter_of(2 + q)]),
    )

    def up_copies(tile):
        all_up[tile, r] = home1[1 + tile]
        yield from over_rows(all_up.at[tile])

    pair_of = (lax.broadcasted_iota(jnp.int32, (256, 128), 0) % 8) // 2

    def placed(sup, value):
        side, pair = PLACE[sup]
        here = low_lanes if side == 0 else jnp.logical_not(low_lanes)
        return jnp.where(here & (pair_of == pair), value, 0.0)

    right_sum = [jnp.zeros((256, 128), F32)]

    def minus_post(home, group, slots):
        parts = halves(home[group].reshape(256, 128))
        for slot in slots:
            if slot is None:
                continue
            sup, second = slot
            at = jnp.minimum(ancestor_of(parent, sup, second), NS - 1)
            value = mm3((post_high[at], post_low[at]), parts)
            right_sum[0] = right_sum[0] - placed(sup, value)

    def right_sides():
        split_d(5)
        yield
        post_both = bulk(post_all.at[pl.ds(0, 31)], post_all.at[pl.ds(0, 31)], post_sems)
        post_both.wait_recv()
        pending.append(post_both)
        for sup in range(NS):
            rows = post_all[:, 2 * sup : 2 * sup + 2, :]
            value = jnp.concatenate([rows] * 4, axis=1).reshape(256, 256)
            high, low = halves(value)
            post_high[sup] = high
            post_low[sup] = low
        yield
        pick_row = lax.broadcasted_iota(jnp.int32, (256, 128), 0)
        pick_col = lax.broadcasted_iota(jnp.int32, (256, 128), 1) % 64 + x * 64
        picker = jnp.where((pick_row == pick_col) & (r == c // 4), 1.0, 0.0).astype(BF16)
        for sup in range(NS):
            value = mm(post_high[sup], picker) + mm(post_low[sup], picker)
            right_sum[0] = right_sum[0] + placed(sup, value)
        yield
        for group in range(3):
            minus_post(home1, group, FIRST[group])

    moved1.append(exchange(all1, home1, 2))

    def later(rounds, tile):
        for _ in range(rounds):
            yield
        yield from share(all1, home1, tile, moved1[tile])

    beside = [later(3, 0), later(4, 1), later(4, 2)]
    run_together(
        (order_a, order_b, sums2[0], sums2[1], up_copies(0), up_copies(1), right_sides()),
        beside,
    )

    for pair in range(16):
        cols = pl.ds(pair * 128, 128)
        even = spread[pair // 2, 2 * (pair % 2)]
        odd = spread[pair // 2, 2 * (pair % 2) + 1]
        wide = low_lanes[0:size]
        for side, value in (
            (0, jnp.where(wide, even, rolled(odd))),
            (1, jnp.where(wide, rolled(even), odd)),
        ):
            high, low = halves(value)
            rows = pl.ds(side * size, size)
            h_high[rows, cols] = high
            h_low[rows, cols] = low
    lane_256 = lax.broadcasted_iota(jnp.int32, (1, 256), 1)
    through = jnp.zeros((256, 256), F32)
    for place in range(width):
        keep = jnp.zeros((1, 256), F32)
        for at, sup in enumerate((2, 3, 0, 1)):
            chosen_here = jnp.int32(0)
            for inner_sup, weight in picks:
                if inner_sup > sup:
                    chosen_here = chosen_here + weight[place] * (parent[sup] == inner_sup).astype(jnp.int32)
            keep = keep + jnp.where(lane_256 // 64 == at, chosen_here.astype(F32), 0.0)
        for row_block in range(8):
            right = jnp.concatenate(
                [all_up[tile, row_block].reshape(256, 128) for tile in range(2)], axis=1
            )
            cols = pl.ds(row_block * 256, 256)
            rows = pl.ds(place * 256, 256)
            through = through + mm3((h_high[rows, cols], h_low[rows, cols]), halves(right * keep))
    moved2 = []
    for group in range(2):
        value = home2[group].reshape(256, 128) - through[:, group * 128 : group * 128 + 128]
        home2[group] = value.reshape(32, 8, 128)
        moved2.append(exchange(all2, home2, group))
    for group in range(2):
        minus_post(home2, group, SECOND[group])
    home2[2] = right_sum[0].reshape(32, 8, 128)
    moved2.append(exchange(all2, home2, 2))

    lane64 = low_lanes[0:64]
    lane8 = low_lanes[0:8]

    def gather_left(everyone, group):
        for pair in range(16):
            even = everyone[group, :, 2 * pair].reshape(64, 128)
            odd = everyone[group, :, 2 * pair + 1].reshape(64, 128)
            cols = pl.ds(pair * 128, 128)
            for side, value in (
                (0, jnp.where(lane64, even, rolled(odd))),
                (1, jnp.where(lane64, rolled(even), odd)),
            ):
                high, low = halves(value)
                l_high[side, 0:64, cols] = high
                l_low[side, 0:64, cols] = low

    def gather_sums(everyone, group):
        for pair in range(16):
            even = jnp.sum(everyone[group, :, 2 * pair], axis=0)
            odd = jnp.sum(everyone[group, :, 2 * pair + 1], axis=0)
            cols = pl.ds(pair * 128, 128)
            blank = jnp.zeros((8, 128), F32)
            for side, value in (
                (0, jnp.where(lane8, even, rolled(odd))),
                (1, jnp.where(lane8, rolled(even), odd)),
            ):
                high, low = halves(jnp.concatenate([value, blank], axis=0))
                x_high[side, :, cols] = high
                x_low[side, :, cols] = low

    def times_d(sup, side, with_sums):
        highs, lows = l_high[side], l_low[side]
        if with_sums:
            highs = jnp.concatenate([highs, x_high[side]], axis=0)
            lows = jnp.concatenate([lows, x_low[side]], axis=0)
        value = mm3((highs, lows), (d_high[sup], d_low[sup]))
        top = value[0:64]
        own_var[sup, :] = own_var[sup, :] + jnp.sum(top * top, axis=0)
        return value

    def put_mean(sup, rows):
        place = PLACE[sup][1]
        mean_out[sup] = rows[2 * place : 2 * place + 2]

    def products(everyone, group, slots, with_sums):
        gather_left(everyone, group)
        for side, slot in enumerate(slots):
            if slot is None:
                continue
            value = times_d(slot[0], side, with_sums)
            if with_sums:
                put_mean(slot[0], value[64:80])

    share2 = [share(all2, home2, tile, moved2[tile]) for tile in range(3)]
    run_together(beside + share2)
    for tile in range(3):
        products(all1, tile, FIRST[tile], False)
    gather_sums(all2, 2)
    for group in range(2):
        products(all2, group, SECOND[group], True)
    for sup in (4, 5):
        side = PLACE[sup][0]
        put_mean(sup, mm3((x_high[side], x_low[side]), (d_high[sup], d_low[sup])))

    copies = []
    for step in range(1, 4):
        copies.append(copy_to(own_var, sums_x.at[step - 1], (y, k, z, (x + step) % 4)))
    for copy in copies:
        copy.wait_recv()
    sums_z[0] = own_var[...] + sums_x[0] + sums_x[1] + sums_x[2]
    copies = []
    for step in range(1, 8):
        copies.append(copy_to(sums_z.at[0], sums_z.at[step], (y, k, (z + step) % 8, x)))
    for copy in copies:
        copy.wait_recv()
    total = sums[...]
    for step in range(8):
        total = total + sums_z[step]
    var_out[...] = total[0:NS]
    while pending:
        pending.pop().wait_send()


def sweep(width, parent, marks, blocks, diag_inv, post):
    any_ = pl.BlockSpec(memory_space=pl.ANY)
    vmem = pl.BlockSpec(memory_space=pltpu.VMEM)
    smem = pl.BlockSpec(memory_space=pltpu.SMEM)
    return pl.pallas_call(
        functools.partial(sweep_kernel, width),
        out_shape=(jax.ShapeDtypeStruct((NS, 2, 256), F32), jax.ShapeDtypeStruct((NS, 256), F32)),
        in_specs=[smem, smem, any_, any_, vmem],
        out_specs=(vmem, vmem),
        scratch_shapes=[
            pltpu.VMEM((3, 4, 2, 256, 128), F32),
            pltpu.VMEM((2, 4, 2, 256, 128), F32),
            pltpu.VMEM((3, 4, 256, 128), F32),
            pltpu.VMEM((2, 4, 256, 128), F32),
            pltpu.VMEM((3, 2, 128, 128), F32),
            pltpu.VMEM((2, 2, 128, 128), F32),
            pltpu.VMEM((3, 2, 256, 128), F32),
            pltpu.VMEM((2, 2, 256, 128), F32),
            pltpu.VMEM((3, 32, 8, 128), F32),
            pltpu.VMEM((3, 32, 8, 128), F32),
            pltpu.VMEM((3, 8, 32, 8, 128), F32),
            pltpu.VMEM((3, 8, 32, 8, 128), F32),
            pltpu.VMEM((2, 8, 32, 8, 128), F32),
            pltpu.VMEM((8, 4, width * 128, 128), F32),
            pltpu.VMEM((3, 2048, 256), F32),
            pltpu.VMEM((NS, 2048, 256), BF16),
            pltpu.VMEM((NS, 2048, 256), BF16),
            pltpu.VMEM((NS, NS, 64, 256), F32),
            pltpu.VMEM((32, 16, 256), F32),
            pltpu.VMEM((NS, 256, 256), BF16),
            pltpu.VMEM((NS, 256, 256), BF16),
            pltpu.VMEM((2, 64, 2048), BF16),
            pltpu.VMEM((2, 64, 2048), BF16),
            pltpu.VMEM((2, 16, 2048), BF16),
            pltpu.VMEM((2, 16, 2048), BF16),
            pltpu.VMEM((width * 256, 2048), BF16),
            pltpu.VMEM((width * 256, 2048), BF16),
            pltpu.VMEM((16, 256), F32),
            pltpu.VMEM((8, 256), F32),
            pltpu.VMEM((8, 256), F32),
            pltpu.VMEM((3, 8, 256), F32),
            pltpu.VMEM((8, 8, 256), F32),
            pltpu.SemaphoreType.DMA((200,)),
            pltpu.SemaphoreType.DMA((200,)),
            pltpu.SemaphoreType.DMA((7,)),
        ],
        compiler_params=pltpu.CompilerParams(
            collective_id=width - 1, has_side_effects=True, vmem_limit_bytes=67_000_000
        ),
        cost_estimate=pl.CostEstimate(flops=12_000_000_000, bytes_accessed=30_000_000, transcendentals=0),
    )(parent, marks, blocks, diag_inv, post)


def count_kernel(parent, count):
    count[0] = sum(inner_flags(parent).values())


def inner_count(parent):
    smem = pl.BlockSpec(memory_space=pltpu.SMEM)
    return pl.pallas_call(
        count_kernel, out_shape=jax.ShapeDtypeStruct((1,), jnp.int32), in_specs=[smem], out_specs=smem
    )(parent)


def body(factor, diag_inv, structure, parent, post):
    marks = jnp.transpose(structure, (0, 2, 1))
    blocks = jnp.transpose(factor, (0, 2, 3, 1))
    mean, variance = lax.cond(
        inner_count(parent)[0] <= 1,
        functools.partial(sweep, 1),
        functools.partial(sweep, 2),
        parent, marks, blocks, diag_inv, jnp.transpose(post, (0, 2, 1)),
    )
    return jnp.transpose(mean, (0, 2, 1)), variance


def solution(mesh):
    finer = Mesh(mesh.devices.reshape(4, 2, 8, 4), ("y", "core", "z", "x"))
    row, col = ("y", "core"), ("z", "x")
    placed = (
        P(None, row, None, col),
        P(None, None, row),
        P(None, None, row),
        P(),
        P(None, row, col),
    )
    return jax.shard_map(
        body,
        mesh=finer,
        in_specs=placed,
        out_specs=(P(None, row, col), P(None, row)),
        check_vma=False,
    )
```
